256 devices in a mesh: groups: 2 (over y), expert: 32 (over z, core), tensor: 4 (over x).
Axes of the slice: x: 4, y: 2, z: 16, core: 2. Of those that a mesh axis runs over, the one named last changes fastest.
The devices are a block of a 4x16x16 slice.
Arguments:
- tokens: bfloat16 [8192, 6144], P(('groups', 'expert', 'tensor')), parts along dimension 0, may hold values from -6 to 6
- expert_ids: int32 [8192, 2], P(('groups', 'expert', 'tensor')), parts along dimension 0, may hold values from 0 to 31, all different within a row; in each aligned block of 32 rows (0 to 31, 32 to 63, ...) at most 4 rows name the same one
- gate_scores: float32 [8192, 2], P(('groups', 'expert', 'tensor')), parts along dimension 0, may hold values from 0.1 to 1
- norm_gain: float32 [6144], replicated, may hold values from 0.1 to 1.9
- w_gate: bfloat16 [32, 6144, 1024], P('expert', None, 'tensor'), may hold values from -0.078125 to 0.078125
- w_up: bfloat16 [32, 6144, 1024], P('expert', None, 'tensor'), may hold values from -0.078125 to 0.078125
- w_down: bfloat16 [32, 1024, 6144], P('expert', 'tensor'), may hold values from -0.1875 to 0.1875
Outputs:
- mixed: bfloat16 [8192, 6144], P(('groups', 'expert', 'tensor')), parts along dimension 0
The draws below stay inside these ranges and needn't reach their ends.
There are 2 independent parts, one for each index of `groups`. The reference program is written for one: setup_inputs(seed, part) draws one part's arguments, and reference() takes and returns one part's arrays. A program takes and returns all parts, laid end to end along the dimension named above; an argument that names none is the same for every part. Nothing has to cross between parts.
Inputs may be any that keep to these rules, and one draw needn't show every extreme that they name: `expert_ids`: each token names 2 different experts. Within the 32 tokens of one device, no expert is named more than 4 times, a bound that some block reaches.
All inputs are finite; a program needn't handle non-finite values.
Results may differ from the reference program's by a relative error of at most 0.011.
Values may be sent and summed in bfloat16 or wider, within the bound.
A program may use at most 64 MiB of HBM per device.

```python
import math
import jax
import jax.numpy as jnp
import numpy as np
from jax import lax

D = 6144
FF = 1024
TOP = 2
TOK_DEV = 32
EXPERTS = 32
CAP = 4
TOKENS = 4096
N_TENSOR = 4


def block_scale(rng, dims, split, low, high):
    loudness, own = 1.0, jax.random.fold_in(rng, 6)
    for position, parts in split:
        draws = jnp.exp(jax.random.uniform(jax.random.fold_in(own, position), (parts,), jnp.float32, low / len(split), high / len(split)))
        loudness = loudness * jnp.repeat(draws, dims[position] // parts).reshape([-1 if axis == position else 1 for axis in range(len(dims))])
    return loudness


def shared_out(rng, own, number, rows, amount, top, limit, slope):
    sequence = jax.random.permutation(rng, amount)
    heavy_load, usual = portions_of(amount, rows * top, limit, slope, True), portions_of(amount, rows * top, limit, slope, False)
    places = jnp.arange(amount)

    def named(lengths, offset_by):
        used = int((lengths > 0).sum())
        fixed = max(1, used // 4)
        moved = fixed + (places - fixed + offset_by * (used - fixed)) % max(1, amount - fixed)
        return jnp.zeros((amount,), jnp.int32).at[sequence[jnp.where(places < fixed, places, moved)]].set(jnp.asarray(lengths, jnp.int32))

    lengths = jnp.where(number % 4 == 0, named(heavy_load, number // 4), named(usual, number - number // 4 - 1))
    mixed = jax.random.permutation(jax.random.fold_in(own, 3), amount)
    giver, sink = mixed[0:amount // 2 * 2:2], mixed[1:amount // 2 * 2:2]
    room = jnp.minimum(lengths[giver] - 1, limit - lengths[sink]) // 2
    room = jnp.where((giver == sequence[0]) | (sink == sequence[0]) | (lengths[sink] == 0), 0, jnp.maximum(room, 0))
    moved = jax.random.randint(jax.random.fold_in(own, 4), (amount // 2,), 0, 1 << 20) % (room + 1)
    lengths = lengths.at[giver].add(-moved).at[sink].add(moved)
    members = jnp.searchsorted(jnp.cumsum(lengths), jnp.arange(rows * top), side="right").astype(jnp.int32)
    listing = members.reshape(top, rows).T
    listing = listing[jax.random.permutation(jax.random.fold_in(own, 1), rows)]
    offset_by = jax.random.randint(jax.random.fold_in(own, 2), (rows, 1), 0, top)
    return jnp.take_along_axis(listing, (jnp.arange(top)[None, :] + offset_by) % top, axis=1)


def portions_of(count, total, most, skew, full):
    portions = [(1 << 20) // math.isqrt(standing ** skew) + 1 for standing in range(1, count + 1)]
    largest = most if full else min(most, max(-(-total // count), total * portions[0] // sum(portions)))
    least = 1 if total - largest >= count - 1 else 0
    holding, rest = [largest] + [least] * (count - 1), total - largest - least * (count - 1)
    while rest > 0:
        movable = [i for i in range(1, count) if holding[i] < largest] or [i for i in range(1, count) if holding[i] < most]
        whole, budget = sum([portions[i] for i in movable]), rest
        for i in movable:
            more = min(most - holding[i], max(1, budget * portions[i] // whole), rest)
            holding[i] = holding[i] + more
            rest = rest - more
    return np.array(holding)


def noise(key, extent, scale, limit, pieces=(), held_as=jnp.bfloat16):
    drawn = jax.random.normal(key, extent, jnp.float32) * scale
    if len(pieces) > 0:
        drawn = block_scale(key, extent, pieces, -0.22, 0.18) * drawn
    return jnp.clip(drawn, min=-limit, max=limit).astype(held_as)


def setup_inputs(seed: int = 0, part: int = 0) -> dict:
    key_list = jax.random.split(jax.random.key(seed), 8)
    part_splits = jax.random.split(jax.random.fold_in(key_list[7], part), 8)
    tokens = noise(part_splits[0], (TOKENS, D), 1.0, 6.0, ((0, 128),))
    expert_ids_keys = jax.random.split(jax.random.fold_in(part_splits[1], 1), TOKENS // TOK_DEV)
    expert_ids_turns = jax.random.permutation(jax.random.fold_in(part_splits[1], 3), TOKENS // TOK_DEV)
    expert_ids = jax.vmap(lambda own, number: shared_out(jax.random.fold_in(part_splits[1], 2), own, number, TOK_DEV, EXPERTS, TOP, CAP, 2))(expert_ids_keys, expert_ids_turns).reshape((TOKENS, TOP))
    gate_scores = jnp.clip(0.1 + 0.9 * jax.random.uniform(part_splits[2], (TOKENS, TOP), jnp.float32) ** block_scale(part_splits[2], (TOKENS, TOP), ((0, 128),), -0.2, 0.2), 0.1, 1.0)
    norm_gain = jnp.clip(1.0 + 0.18 * jax.random.normal(key_list[3], (D,), jnp.float32), 0.1, 1.9)
    w_gate = noise(key_list[4], (EXPERTS, D, FF), D ** -0.5, 0.078125, ((0, 32), (2, 4)))
    w_up = noise(key_list[5], (EXPERTS, D, FF), D ** -0.5, 0.078125, ((0, 32), (2, 4)))
    w_down = noise(key_list[6], (EXPERTS, FF, D), FF ** -0.5, 0.1875, ((0, 32), (1, 4)))
    return {"tokens": tokens, "expert_ids": expert_ids, "gate_scores": gate_scores, "norm_gain": norm_gain, "w_gate": w_gate, "w_up": w_up, "w_down": w_down}


def reference(tokens, expert_ids, gate_scores, norm_gain, w_gate, w_up, w_down):
    values = tokens.astype(jnp.float32)
    scale = lax.rsqrt(lax.optimization_barrier(jnp.mean(values * values, axis=-1, keepdims=True)) + 1e-05)
    normed = (values * scale * norm_gain).astype(jnp.bfloat16)
    blocks = TOKENS // TOK_DEV
    assigned = TOK_DEV * TOP
    block_ids = expert_ids.reshape(blocks, assigned).astype(jnp.int32)
    onehot = (block_ids[:, :, None] == jnp.arange(EXPERTS, dtype=jnp.int32)[None, None, :]).astype(jnp.int32)
    earlier = jnp.cumsum(onehot, axis=1) - onehot
    slot = lax.optimization_barrier(jnp.sum(earlier * onehot, axis=-1)).astype(jnp.int32)
    target = (block_ids * CAP + slot).astype(jnp.int32)
    repeated = jnp.repeat(normed.reshape(blocks, TOK_DEV, D), TOP, axis=1)
    block_index = jnp.broadcast_to(jnp.arange(blocks, dtype=jnp.int32)[:, None], (blocks, assigned))
    buffer = jnp.zeros((blocks, EXPERTS * CAP, D), jnp.bfloat16).at[block_index, target].set(repeated)
    per_expert = buffer.reshape(blocks, EXPERTS, CAP, D).transpose(1, 0, 2, 3).reshape(EXPERTS, blocks * CAP, D)
    group = FF // N_TENSOR

    def expert_fn(operands):
        rows, gate_w, up_w, down_w = operands
        gate = jnp.dot(rows, gate_w, preferred_element_type=jnp.float32)
        up = jnp.dot(rows, up_w, preferred_element_type=jnp.float32)
        hidden = (jax.nn.silu(gate) * up).astype(jnp.bfloat16)
        total = jnp.zeros((rows.shape[0], D), jnp.float32)
        for index in range(N_TENSOR):
            part = jnp.dot(hidden[:, index * group:(index + 1) * group], down_w[index * group:(index + 1) * group], preferred_element_type=jnp.float32)
            total = total + part.astype(jnp.bfloat16).astype(jnp.float32)
        return total.astype(jnp.bfloat16)
    outputs = lax.map(expert_fn, (per_expert, w_gate, w_up, w_down))
    back = outputs.reshape(EXPERTS, blocks, CAP, D).transpose(1, 0, 2, 3).reshape(blocks, EXPERTS * CAP, D)
    picked = jnp.take_along_axis(back, target[:, :, None], axis=1).astype(jnp.float32)
    picked = picked.reshape(TOKENS, TOP, D)
    mixed = lax.optimization_barrier(jnp.sum(gate_scores[:, :, None] * picked, axis=1))
    return mixed.astype(jnp.bfloat16)
```

```python
import functools

import jax
import jax.numpy as jnp
from jax import lax
from jax.experimental import pallas as pl
from jax.experimental.pallas import tpu as pltpu
from jax.sharding import PartitionSpec as P

MESH = pl.DeviceIdType.MESH
F32, BF16 = jnp.float32, jnp.bfloat16
PARTS = 3
DMA = pltpu.SemaphoreType.DMA


def kernel(E, NX, rows, width, norm, meta, wg_in, wu_in, wd_in, out,
           T, M, FS, G, WG, WU, WD, ACC, HID, PB, OPP, RX, R, FR, C, CP, CR, RZ,
           wsem, zs, zr, ps, pr, zms, zmr, pms, pmr, fs, fr, xs, xr, xfs, xfr,
           os_, or_, ms_, mr_, bs, br, cs_, cr_, rs, rr):
    Z = E // 2
    HOP = Z // 4
    cap = 4 * rows // E
    blk = 2 * cap
    fw = width // PARTS
    hid = WG.shape[1]
    e = lax.axis_index("expert")
    x = lax.axis_index("tensor")
    c = lax.rem(e, 2)
    sgn = (1, -1)

    def at_z(k):
        return {"expert": lax.rem(e + 2 * k + 2 * E, E)}

    partner = {"expert": e + 1 - 2 * c}
    side_dev = ({"tensor": lax.rem(x + 1, NX)}, {"tensor": lax.rem(x + NX - 1, NX)})

    def cols(f):
        return pl.ds(pl.multiple_of(f * fw, fw), fw)

    def rcopy(src, dst, s, r, dev):
        return pltpu.make_async_remote_copy(src_ref=src, dst_ref=dst, send_sem=s, recv_sem=r,
                                            device_id=dev, device_id_type=MESH)

    def each_part(body):
        def step(f, carry):
            body(f)
            return carry
        lax.fori_loop(0, PARTS, step, 0)

    def idx(d, j):
        return 0 if j == 0 else 2 * j - 1 + d

    def z_meta(d, j):
        return rcopy(meta if j == 0 else M.at[idx(d, j), 0], M.at[idx(d, j + 1), 0],
                     zms.at[d, j], zmr.at[d, j], at_z(sgn[d]))

    def p_meta(o):
        return rcopy(meta if o == 0 else M.at[o, 0], M.at[o, 1], pms.at[o], pmr.at[o], partner)

    def z_tok(d, j, f):
        src = norm.at[:, cols(f)] if j == 0 else T.at[idx(d, j), 0, :, cols(f)]
        return rcopy(src, T.at[idx(d, j + 1), 0, :, cols(f)], zs.at[d, j, f], zr.at[d, j, f], at_z(sgn[d]))

    def p_tok(o, f):
        src = norm.at[:, cols(f)] if o == 0 else T.at[o, 0, :, cols(f)]
        return rcopy(src, T.at[o, 1, :, cols(f)], ps.at[o, f], pr.at[o, f], partner)

    def far(d, i, f):
        if i == HOP:
            return rcopy(FS.at[c, i - 1, :, cols(f)], G.at[0, Z - 1, :, cols(f)],
                         fs.at[0, i - 1, f], fr.at[0, i - 1, f],
                         {"expert": lax.rem(e + 2 * i * (1 - 2 * c) + 2 * E, E)})
        return rcopy(FS.at[d, i - 1, :, cols(f)], G.at[0, idx(d, HOP + i), :, cols(f)],
                     fs.at[d, i - 1, f], fr.at[d, i - 1, f], at_z(sgn[d] * i))

    groups = [(0, 3)] + [(2 * j - 1, 2 * j + 1) for j in range(2, 2 * HOP - 1)] + [(Z - 3, Z)]
    NG = len(groups)

    def half(g, side):
        b0, b1 = groups[g]
        cut = b0 + 2 if g == 0 else b0 + 1
        return slice(b0, cut) if side == 0 else slice(cut, b1)

    def xsend(g, side):
        b = slice(*groups[g])
        return rcopy(G.at[0, b], G.at[1 + side, b], xs.at[g, side], xr.at[g, side], side_dev[side])

    def xfwd(g, side):
        b = half(g, side)
        return rcopy(G.at[1 + side, b], G.at[3, b], xfs.at[g, side], xfr.at[g, side], side_dev[side])

    def opp(g, side):
        b = half(g, side)
        return rcopy(PB.at[3, b], OPP.at[b], os_.at[g, side], or_.at[g, side], side_dev[side])

    def main(g, side):
        b = slice(*groups[g])
        return rcopy(PB.at[2 - side, b], RX.at[side, b], ms_.at[g, side], mr_.at[g, side], side_dev[side])

    def back(d, i):
        if i == HOP:
            return rcopy(R.at[Z - 1], FR.at[c, i - 1], bs.at[0, i - 1], br.at[0, i - 1],
                         {"expert": lax.rem(e - 2 * i * (1 - 2 * c) + 2 * E, E)})
        return rcopy(R.at[idx(d, HOP + i)], FR.at[d, i - 1], bs.at[d, i - 1], br.at[d, i - 1],
                     at_z(-sgn[d] * i))

    def p_con(o, f):
        return rcopy(CP.at[o, :, cols(f)], CR.at[o, :, cols(f)], cs_.at[o, f], cr_.at[o, f], partner)

    def ring(d, j, f):
        return rcopy(C.at[idx(d, j), :, cols(f)], RZ.at[d, j - 1, :, cols(f)],
                     rs.at[d, j - 1, f], rr.at[d, j - 1, f], at_z(-sgn[d]))

    lane = lax.broadcasted_iota(jnp.int32, (1, 128), 1)

    def picks(o, n, first, scored):
        def both(r):
            return jnp.where(lane < rows, M[o, 0, r:r + 1, :], M[o, 1, r:r + 1, :])
        r = lax.broadcasted_iota(jnp.int32, (n * blk, 128), 0)
        ln = lax.broadcasted_iota(jnp.int32, (n * blk, 128), 1)
        ex = first(r // blk)
        ex = jnp.where(ex >= E, ex - E, ex)
        ex = jnp.where(ex < 0, ex + E, ex)
        slot = (cap * ex + lax.rem(r, cap)).astype(F32)
        mine = (lax.rem(r, blk) // cap) == (ln // rows)
        one = jnp.ones((n * blk, 128), F32)
        a, b = (both(2), both(3)) if scored else (one, one)
        val = jnp.where(both(0) == slot, a, 0.0) + jnp.where(both(1) == slot, b, 0.0)
        return jnp.where(mine, val, 0.0)[:, :2 * rows].astype(BF16)

    def own(o, scored):
        return picks(o, 1, lambda i: i + e, scored)

    def beyond(o, d, scored):
        return picks(o, HOP, lambda i: e + 2 * sgn[d] * (i + 1), scored)

    def select(lhs, o, f):
        return jnp.dot(lhs, T[o, :, :, cols(f)].reshape(2 * rows, fw), preferred_element_type=F32)

    def ffn_in(b0, b1):
        n = NX * (b1 - b0) * blk
        kc = width // 6
        ACC[:, 0:n] = jnp.zeros((2, n, hid), F32)

        def step(k, carry):
            ks = pl.ds(pl.multiple_of(k * kc, kc), kc)
            lhs = G[:, b0:b1, :, ks].reshape(n, kc)
            ACC[0, 0:n] += jnp.dot(lhs, WG[ks, :], preferred_element_type=F32)
            ACC[1, 0:n] += jnp.dot(lhs, WU[ks, :], preferred_element_type=F32)
            return carry
        lax.fori_loop(0, 6, step, 0)
        gate = ACC[0, 0:n]
        h = gate / (1.0 + jnp.exp(-gate)) * ACC[1, 0:n]
        HID[:, b0:b1] = h.astype(BF16).reshape(NX, b1 - b0, blk, hid)

    def ffn_out(g):
        b0, b1 = groups[g]
        n = NX * (b1 - b0) * blk
        kc = width // 6
        lhs = HID[:, b0:b1].reshape(n, hid)

        def step(k, carry):
            ks = pl.ds(pl.multiple_of(k * kc, kc), kc)
            PB[:, b0:b1, :, ks] = jnp.dot(lhs, WD[:, ks], preferred_element_type=F32).astype(BF16).reshape(NX, b1 - b0, blk, kc)
            return carry
        lax.fori_loop(0, 6, step, 0)

    weights = [pltpu.make_async_copy(wg_in.at[0], WG, wsem.at[0]),
               pltpu.make_async_copy(wu_in.at[0], WU, wsem.at[1]),
               pltpu.make_async_copy(wd_in.at[0], WD, wsem.at[2])]
    for w in weights:
        w.start()
    barrier = pltpu.get_barrier_semaphore()
    peers = [at_z(s * k) for k in range(1, HOP + 1) for s in sgn] + list(side_dev) + [partner]
    for dev in peers:
        pl.semaphore_signal(barrier, inc=1, device_id=dev, device_id_type=MESH)
    T[0, 0] = norm[...]
    M[0, 0] = meta[...]
    FR[1 - c, HOP - 1] = jnp.zeros((blk, width), BF16)
    pl.semaphore_wait(barrier, len(peers))

    sent = []

    def go(make, *a):
        make(*a).start()
        sent.append((make, a, False))

    def note(make, *a):
        sent.append((make, a, True))

    for d in (0, 1):
        go(z_meta, d, 0)
    go(p_meta, 0)

    def first(f):
        p_tok(0, f).start()
        z_tok(0, 0, f).start()
        z_tok(1, 0, f).start()
    each_part(first)
    note(p_tok, 0)
    note(z_tok, 0, 0)
    note(z_tok, 1, 0)

    p_meta(0).wait_recv()
    lhs0 = own(0, False)

    def sel0(f):
        p_tok(0, f).wait_recv()
        G[0, 0, :, cols(f)] = select(lhs0, 0, f).astype(BF16)
    each_part(sel0)

    def spread(g):
        go(xsend, g, 0)
        go(xsend, g, 1)

    def forward(g):
        for side in (0, 1):
            xsend(g, side).wait_recv()
            go(xfwd, g, side)

    def gathered(g):
        for side in (0, 1):
            xfwd(g, side).wait_recv()

    for j in range(1, HOP + 1):
        for d in (0, 1):
            z_meta(d, j - 1).wait_recv()
            if j < HOP:
                go(z_meta, d, j)
            go(p_meta, idx(d, j))

        def hop(f):
            for d in (0, 1):
                z_tok(d, j - 1, f).wait_recv()
                if j < HOP:
                    z_tok(d, j, f).start()
                p_tok(idx(d, j), f).start()
        each_part(hop)
        for d in (0, 1):
            if j < HOP:
                note(z_tok, d, j)
            note(p_tok, idx(d, j))
        for d in (0, 1):
            p_meta(idx(d, j)).wait_recv()
        lhs = [own(idx(d, j), False) for d in (0, 1)]
        if j == HOP:
            lhs = [jnp.concatenate([lhs[d], beyond(idx(d, j), d, False)], axis=0) for d in (0, 1)]

        def sel(f):
            for d in (0, 1):
                o = idx(d, j)
                p_tok(o, f).wait_recv()
                got = select(lhs[d], o, f).astype(BF16)
                G[0, o, :, cols(f)] = got[:blk]
                if j == HOP:
                    FS[d, :, :, cols(f)] = got[blk:].reshape(HOP, blk, fw)
            if j == HOP:
                for i in range(1, HOP):
                    for d in (0, 1):
                        far(d, i, f).start()
                far(0, HOP, f).start()
        each_part(sel)
        if j == HOP:
            for i in range(1, HOP):
                for d in (0, 1):
                    note(far, d, i)
            note(far, 0, HOP)
        spread(j - 1)
        if j > 1:
            forward(j - 2)

    for w in weights:
        w.wait()
    gathered(0)
    gathered(1)
    ffn_in(0, 5)
    for i in range(1, HOP):
        for d in (0, 1):
            each_part(lambda f: far(d, i, f).wait_recv())
        if i == HOP - 1:
            each_part(lambda f: far(0, HOP, f).wait_recv())
        spread(HOP + i - 1)
        forward(HOP + i - 2)
        if i == 2:
            gathered(2)
            gathered(3)
            ffn_in(5, 9)
    forward(NG - 1)
    gathered(4)
    gathered(5)
    ffn_in(9, 13)

    def begin(g):
        ffn_out(g)
        go(opp, g, 0)
        go(opp, g, 1)

    def middle(g):
        for side in (0, 1):
            b = half(g, side)
            n = b.stop - b.start
            opp(g, side).wait_recv()

            def add(f):
                PB[2 - side, b, :, cols(f)] = (PB[2 - side, b, :, cols(f)].astype(F32) + OPP[b, :, cols(f)].astype(F32)).astype(BF16)
            each_part(add)
            go(main, g, side)

    def finish(g):
        b = slice(*groups[g])
        for side in (0, 1):
            main(g, side).wait_recv()

        def add(f):
            R[b, :, cols(f)] = (PB[0, b, :, cols(f)].astype(F32) + RX[0, b, :, cols(f)].astype(F32)
                                + RX[1, b, :, cols(f)].astype(F32)).astype(BF16)
        each_part(add)

    def far_back(g):
        i = g - HOP + 1
        for d in (0, 1):
            go(back, d, i)
        if g == NG - 1:
            go(back, 0, HOP)

    def weigh(lhs, rhs):
        return lax.dot_general(lhs, rhs, (((0,), (0,)), ((), ())), preferred_element_type=F32)

    def give(j):
        for d in ((0, 1) if j > 0 else (0,)):
            o = idx(d, j)
            w_own = own(o, True)
            w_far = None
            if j == HOP:
                w_far = beyond(o, d, True)
                for i in range(1, HOP):
                    back(d, i).wait_recv()
                if d == 0:
                    back(0, HOP).wait_recv()

            def step(f):
                u = weigh(w_own, R[o, :, cols(f)])
                if j == HOP:
                    u = u + weigh(w_far, FR[d, :, :, cols(f)].reshape(HOP * blk, fw))
                C[o, :, cols(f)] = u[:rows].astype(BF16)
                CP[o, :, cols(f)] = u[rows:].astype(BF16)
                p_con(o, f).start()
            each_part(step)
            note(p_con, o)

    def pass_on(j):
        def step(f):
            for d in (0, 1):
                o = idx(d, j)
                p_con(o, f).wait_recv()
                v = C[o, :, cols(f)].astype(F32) + CR[o, :, cols(f)].astype(F32)
                if j < HOP:
                    ring(d, j + 1, f).wait_recv()
                    v = v + RZ[d, j, :, cols(f)].astype(F32)
                C[o, :, cols(f)] = v.astype(BF16)
                ring(d, j, f).start()
        each_part(step)
        note(ring, 0, j)
        note(ring, 1, j)

    begin(4)
    begin(5)
    gathered(6)
    ffn_in(13, 16)
    begin(6)
    middle(4)
    middle(5)
    begin(3)
    middle(6)
    finish(4)
    far_back(4)
    finish(5)
    far_back(5)
    middle(3)
    finish(6)
    far_back(6)
    begin(2)
    finish(3)
    middle(2)
    begin(1)
    give(4)
    pass_on(4)
    finish(2)
    give(3)
    middle(1)
    begin(0)
    pass_on(3)
    finish(1)
    give(2)
    middle(0)
    pass_on(2)
    finish(0)
    give(1)
    give(0)
    pass_on(1)

    def last(f):
        p_con(0, f).wait_recv()
        ring(0, 1, f).wait_recv()
        ring(1, 1, f).wait_recv()
        out[:, cols(f)] = (C[0, :, cols(f)].astype(F32) + CR[0, :, cols(f)].astype(F32)
                           + RZ[0, 0, :, cols(f)].astype(F32) + RZ[1, 0, :, cols(f)].astype(F32)).astype(BF16)
    each_part(last)

    for make, a, looped in sent:
        if looped:
            each_part(lambda f: make(*a, f).wait_send())
        else:
            make(*a).wait_send()


def on_device(tokens, expert_ids, gate_scores, norm_gain, w_gate, w_up, w_down):
    rows, width = tokens.shape
    E, NX = lax.axis_size("expert"), lax.axis_size("tensor")
    cap = 4 * rows // E
    Z, HOP, blk, hid = E // 2, E // 8, 2 * cap, w_gate.shape[2]
    values = tokens.astype(F32)
    scale = lax.rsqrt(jnp.mean(values * values, axis=-1, keepdims=True) + 1e-05)
    normed = (values * scale * norm_gain).astype(BF16)
    flat = expert_ids.reshape(-1)
    n = flat.shape[0]
    order = jnp.arange(n, dtype=jnp.int32)
    same = (flat[:, None] == flat[None, :]) & (order[None, :] < order[:, None])
    target = (flat * cap + jnp.sum(same.astype(jnp.int32), axis=1)).reshape(rows, -1).astype(F32)
    info = jnp.concatenate([target.T, gate_scores.T], axis=0)
    info = jnp.concatenate([info, info], axis=1)
    meta = jnp.full((8, 128), -1.0, F32).at[:4, :2 * rows].set(info)
    NG, NO = 2 * HOP - 1, 2 * HOP + 1
    v = lambda *s: pltpu.VMEM(s, BF16)
    return pl.pallas_call(
        functools.partial(kernel, E, NX, rows, width),
        out_shape=jax.ShapeDtypeStruct((rows, width), BF16),
        in_specs=[pl.BlockSpec(memory_space=pltpu.VMEM)] * 2 + [pl.BlockSpec(memory_space=pl.ANY)] * 3,
        out_specs=pl.BlockSpec(memory_space=pltpu.VMEM),
        scratch_shapes=[
            v(NO, 2, rows, width),
            pltpu.VMEM((NO, 2, 8, 128), F32),
            v(2, HOP, blk, width),
            v(NX, Z, blk, width),
            v(width, hid), v(width, hid), v(hid, width),
            pltpu.VMEM((2, NX * 5 * blk, hid), F32),
            v(NX, Z, blk, hid),
            v(NX, Z, blk, width),
            v(Z, blk, width),
            v(2, Z, blk, width),
            v(Z, blk, width),
            v(2, HOP, blk, width),
            v(NO, rows, width), v(NO, rows, width), v(NO, rows, width),
            v(2, HOP, rows, width),
            DMA((3,)),
            DMA((2, HOP, PARTS)), DMA((2, HOP, PARTS)), DMA((NO, PARTS)), DMA((NO, PARTS)),
            DMA((2, HOP)), DMA((2, HOP)), DMA((NO,)), DMA((NO,)),
            DMA((2, HOP, PARTS)), DMA((2, HOP, PARTS)),
            DMA((NG, 2)), DMA((NG, 2)), DMA((NG, 2)), DMA((NG, 2)),
            DMA((NG, 2)), DMA((NG, 2)), DMA((NG, 2)), DMA((NG, 2)),
            DMA((2, HOP)), DMA((2, HOP)),
            DMA((NO, PARTS)), DMA((NO, PARTS)),
            DMA((2, HOP, PARTS)), DMA((2, HOP, PARTS)),
        ],
        compiler_params=pltpu.CompilerParams(collective_id=0, has_side_effects=True, vmem_limit_bytes=63 * 1024 * 1024),
    )(normed, meta, w_gate, w_up, w_down)


def solution(mesh):
    return jax.shard_map(
        on_device,
        mesh=mesh,
        in_specs=(
            P(("groups", "expert", "tensor"), None),
            P(("groups", "expert", "tensor"), None),
            P(("groups", "expert", "tensor"), None),
            P(),
            P("expert", None, "tensor"),
            P("expert", None, "tensor"),
            P("expert", "tensor", None),
        ),
        out_specs=P(("groups", "expert", "tensor"), None),
        check_vma=False,
    )
```

```python
import functools

import jax
import jax.numpy as jnp
from jax import lax
from jax.experimental import pallas as pl
from jax.experimental.pallas import tpu as pltpu
from jax.sharding import PartitionSpec as P

MESH = pl.DeviceIdType.MESH
F32, BF16 = jnp.float32, jnp.bfloat16
PARTS = 3
DMA = pltpu.SemaphoreType.DMA


def kernel(E, NX, rows, width, tokens, ids, scores, gain, wg_in, wu_in, wd_in, out,
           T, M, FS, G, WG, WU, WD, ACC, HID, PB, OPP, RX, R, FR, C, CP, CR, RZ,
           wsem, zs, zr, ps, pr, zms, zmr, pms, pmr, fs, fr, xs, xr, xfs, xfr,
           os_, or_, ms_, mr_, bs, br, cs_, cr_, rs, rr):
    Z = E // 2
    HOP = Z // 4
    cap = 4 * rows // E
    blk = 2 * cap
    fw = width // PARTS
    hid = WG.shape[1]
    e = lax.axis_index("expert")
    x = lax.axis_index("tensor")
    c = lax.rem(e, 2)
    sgn = (1, -1)

    def at_z(k):
        return {"expert": lax.rem(e + 2 * k + 2 * E, E)}

    partner = {"expert": e + 1 - 2 * c}
    side_dev = ({"tensor": lax.rem(x + 1, NX)}, {"tensor": lax.rem(x + NX - 1, NX)})

    def cols(f):
        return pl.ds(pl.multiple_of(f * fw, fw), fw)

    def rcopy(src, dst, s, r, dev):
        return pltpu.make_async_remote_copy(src_ref=src, dst_ref=dst, send_sem=s, recv_sem=r,
                                            device_id=dev, device_id_type=MESH)

    def each_part(body):
        def step(f, carry):
            body(f)
            return carry
        lax.fori_loop(0, PARTS, step, 0)

    def idx(d, j):
        return 0 if j == 0 else 2 * j - 1 + d

    def z_meta(d, j):
        return rcopy(M.at[idx(d, j), 0], M.at[idx(d, j + 1), 0],
                     zms.at[d, j], zmr.at[d, j], at_z(sgn[d]))

    def p_meta(o):
        return rcopy(M.at[o, 0], M.at[o, 1], pms.at[o], pmr.at[o], partner)

    def z_tok(d, j, f):
        return rcopy(T.at[idx(d, j), 0, :, cols(f)], T.at[idx(d, j + 1), 0, :, cols(f)], zs.at[d, j, f], zr.at[d, j, f], at_z(sgn[d]))

    def p_tok(o, f):
        return rcopy(T.at[o, 0, :, cols(f)], T.at[o, 1, :, cols(f)], ps.at[o, f], pr.at[o, f], partner)

    def far(d, i, f):
        if i == HOP:
            return rcopy(FS.at[c, i - 1, :, cols(f)], G.at[0, Z - 1, :, cols(f)],
                         fs.at[0, i - 1, f], fr.at[0, i - 1, f],
                         {"expert": lax.rem(e + 2 * i * (1 - 2 * c) + 2 * E, E)})
        return rcopy(FS.at[d, i - 1, :, cols(f)], G.at[0, idx(d, HOP + i), :, cols(f)],
                     fs.at[d, i - 1, f], fr.at[d, i - 1, f], at_z(sgn[d] * i))

    mid, NB = 2 * HOP + 1, Z
    items = [(slice(0, 1), slice(0, width))]
    items += [(slice(2 * j - 1, 2 * j + 1), slice(0, width)) for j in range(1, HOP + 1)]
    items += [(slice(mid, NB), slice(f * fw, (f + 1) * fw)) for f in range(PARTS)]
    FAR = HOP + 1

    def half(g, side):
        b = items[g][0]
        cut = b.start if g == 0 else (b.start + b.stop + 1) // 2
        return slice(b.start, cut) if side == 0 else slice(cut, b.stop)

    def sides(g):
        return [s for s in (0, 1) if half(g, s).stop > half(g, s).start]

    def xsend(g, side):
        b, k = items[g]
        return rcopy(G.at[0, b, :, k], G.at[1 + side, b, :, k], xs.at[g, side], xr.at[g, side], side_dev[side])

    def xfwd(g, side):
        b, k = half(g, side), items[g][1]
        return rcopy(G.at[1 + side, b, :, k], G.at[3, b, :, k], xfs.at[g, side], xfr.at[g, side], side_dev[side])

    def opp(g, side):
        b, k = half(g, side), items[g][1]
        return rcopy(PB.at[3, b, :, k], OPP.at[b, :, k], os_.at[g, side], or_.at[g, side], side_dev[side])

    def main(g, side):
        b, k = items[g]
        return rcopy(PB.at[2 - side, b, :, k], RX.at[side, b, :, k], ms_.at[g, side], mr_.at[g, side], side_dev[side])

    def back(d, i, f):
        if i == HOP:
            return rcopy(R.at[Z - 1, :, cols(f)], FR.at[c, i - 1, :, cols(f)], bs.at[0, i - 1, f], br.at[0, i - 1, f],
                         {"expert": lax.rem(e - 2 * i * (1 - 2 * c) + 2 * E, E)})
        return rcopy(R.at[idx(d, HOP + i), :, cols(f)], FR.at[d, i - 1, :, cols(f)],
                     bs.at[d, i - 1, f], br.at[d, i - 1, f], at_z(-sgn[d] * i))

    def p_con(o, f):
        return rcopy(CP.at[o, :, cols(f)], CR.at[o, :, cols(f)], cs_.at[o, f], cr_.at[o, f], partner)

    def ring(d, j, f):
        return rcopy(C.at[idx(d, j), :, cols(f)], RZ.at[d, j - 1, :, cols(f)],
                     rs.at[d, j - 1, f], rr.at[d, j - 1, f], at_z(-sgn[d]))

    lane = lax.broadcasted_iota(jnp.int32, (1, 128), 1)

    def picks(o, n, first, scored):
        def both(r):
            return jnp.where(lane < rows, M[o, 0, r:r + 1, :], M[o, 1, r:r + 1, :])
        r = lax.broadcasted_iota(jnp.int32, (n * blk, 128), 0)
        ln = lax.broadcasted_iota(jnp.int32, (n * blk, 128), 1)
        ex = first(r // blk)
        ex = jnp.where(ex >= E, ex - E, ex)
        ex = jnp.where(ex < 0, ex + E, ex)
        slot = (cap * ex + lax.rem(r, cap)).astype(F32)
        mine = (lax.rem(r, blk) // cap) == (ln // rows)
        one = jnp.ones((n * blk, 128), F32)
        a, b = (both(2), both(3)) if scored else (one, one)
        val = jnp.where(both(0) == slot, a, 0.0) + jnp.where(both(1) == slot, b, 0.0)
        return jnp.where(mine, val, 0.0)[:, :2 * rows].astype(BF16)

    def own(o, scored):
        return picks(o, 1, lambda i: i + e, scored)

    def beyond(o, d, scored):
        return picks(o, HOP, lambda i: e + 2 * sgn[d] * (i + 1), scored)

    def select(lhs, o, f):
        return jnp.dot(lhs, T[o, :, :, cols(f)].reshape(2 * rows, fw), preferred_element_type=F32)

    kc = fw // 2

    def ffn_in(b, k, fresh=True, done=True):
        n = NX * (b.stop - b.start) * blk
        if fresh:
            ACC[:, 0:n] = jnp.zeros((2, n, hid), F32)

        def step(i, carry):
            ks = pl.ds(pl.multiple_of(k.start + i * kc, kc), kc)
            lhs = G[:, b, :, ks].reshape(n, kc)
            ACC[0, 0:n] += jnp.dot(lhs, WG[ks, :], preferred_element_type=F32)
            ACC[1, 0:n] += jnp.dot(lhs, WU[ks, :], preferred_element_type=F32)
            return carry
        lax.fori_loop(0, (k.stop - k.start) // kc, step, 0)
        if done:
            gate = ACC[0, 0:n]
            h = gate / (1.0 + jnp.exp(-gate)) * ACC[1, 0:n]
            HID[:, b] = h.astype(BF16).reshape(NX, b.stop - b.start, blk, hid)

    def ffn_out(g):
        b, k = items[g]
        n = NX * (b.stop - b.start) * blk
        lhs = HID[:, b].reshape(n, hid)

        def step(i, carry):
            ks = pl.ds(pl.multiple_of(k.start + i * kc, kc), kc)
            PB[:, b, :, ks] = jnp.dot(lhs, WD[:, ks], preferred_element_type=F32).astype(BF16).reshape(NX, b.stop - b.start, blk, kc)
            return carry
        lax.fori_loop(0, (k.stop - k.start) // kc, step, 0)

    barrier = pltpu.get_barrier_semaphore()
    peers = [at_z(s * k) for k in range(1, HOP + 1) for s in sgn] + list(side_dev) + [partner]
    for dev in peers:
        pl.semaphore_signal(barrier, inc=1, device_id=dev, device_id_type=MESH)
    weights = [pltpu.make_async_copy(wg_in.at[0], WG, wsem.at[0]),
               pltpu.make_async_copy(wu_in.at[0], WU, wsem.at[1]),
               pltpu.make_async_copy(wd_in.at[0], WD, wsem.at[2])]
    for w in weights:
        w.start()

    row_t = lax.broadcasted_iota(jnp.int32, (rows, rows), 0)
    col_t = lax.broadcasted_iota(jnp.int32, (rows, rows), 1)
    named = [ids[k:k + 1, :].astype(F32) for k in (0, 1)]
    stood = [jnp.sum(jnp.where(row_t == col_t, r, 0.0), axis=1, keepdims=True) for r in named]
    M[0, 0] = jnp.zeros((8, 128), F32)
    for k in (0, 1):
        ahead = [jnp.where((q == named[k]) & (row_t < col_t), 1.0, 0.0) for q in stood]
        M[0, 0, k:k + 1, 0:rows] = named[k] * cap + jnp.sum(ahead[0] + ahead[1], axis=0, keepdims=True)
        M[0, 0, 2 + k:3 + k, 0:rows] = scores[k:k + 1, :]
    once = M[0, 0]
    M[0, 0] = jnp.where(lane < 2 * rows, once + pltpu.roll(once, rows, 1), -1.0)

    total = jnp.zeros((rows, 1), F32)
    for k in range(0, width, kc):
        t = tokens[:, k:k + kc].astype(F32)
        total = total + jnp.sum(t * t, axis=1, keepdims=True)
    scale = lax.rsqrt(total / width + 1e-05)
    for k in range(0, width, kc):
        T[0, 0, :, k:k + kc] = (tokens[:, k:k + kc].astype(F32) * scale * gain[:, k:k + kc]).astype(BF16)
    FR[1 - c, HOP - 1] = jnp.zeros((blk, width), BF16)
    pl.semaphore_wait(barrier, len(peers))

    sent = []

    def go(make, *a):
        make(*a).start()
        sent.append((make, a, False))

    def note(make, *a):
        sent.append((make, a, True))

    for d in (0, 1):
        go(z_meta, d, 0)
    go(p_meta, 0)

    def first(f):
        p_tok(0, f).start()
        z_tok(0, 0, f).start()
        z_tok(1, 0, f).start()
    each_part(first)
    note(p_tok, 0)
    note(z_tok, 0, 0)
    note(z_tok, 1, 0)

    p_meta(0).wait_recv()
    lhs0 = own(0, False)

    def sel0(f):
        p_tok(0, f).wait_recv()
        G[0, 0, :, cols(f)] = select(lhs0, 0, f).astype(BF16)
    each_part(sel0)

    def spread(g):
        go(xsend, g, 0)
        go(xsend, g, 1)

    def forward(g):
        for side in (0, 1):
            xsend(g, side).wait_recv()
            if side in sides(g):
                go(xfwd, g, side)

    def gathered(g):
        for side in sides(g):
            xfwd(g, side).wait_recv()

    spread(0)
    for j in range(1, HOP + 1):
        for d in (0, 1):
            z_meta(d, j - 1).wait_recv()
            if j < HOP:
                go(z_meta, d, j)
            go(p_meta, idx(d, j))

        def hop(f):
            for d in (0, 1):
                z_tok(d, j - 1, f).wait_recv()
                if j < HOP:
                    z_tok(d, j, f).start()
                p_tok(idx(d, j), f).start()
        each_part(hop)
        for d in (0, 1):
            if j < HOP:
                note(z_tok, d, j)
            note(p_tok, idx(d, j))
        for d in (0, 1):
            p_meta(idx(d, j)).wait_recv()
        lhs = [own(idx(d, j), False) for d in (0, 1)]
        if j == HOP:
            lhs = [jnp.concatenate([lhs[d], beyond(idx(d, j), d, False)], axis=0) for d in (0, 1)]

        def sel(f):
            for d in (0, 1):
                o = idx(d, j)
                p_tok(o, f).wait_recv()
                got = select(lhs[d], o, f).astype(BF16)
                G[0, o, :, cols(f)] = got[:blk]
                if j == HOP:
                    FS[d, :, :, cols(f)] = got[blk:].reshape(HOP, blk, fw)
            if j == HOP:
                for i in range(1, HOP):
                    for d in (0, 1):
                        far(d, i, f).start()
                far(0, HOP, f).start()
        each_part(sel)
        if j == HOP:
            for i in range(1, HOP):
                for d in (0, 1):
                    note(far, d, i)
            note(far, 0, HOP)
        spread(j)
        forward(j - 1)

    for w in weights:
        w.wait()
    full = slice(0, width)
    for g in range(HOP - 1):
        gathered(g)
    ffn_in(slice(0, 2 * HOP - 3), full)
    for f in range(PARTS):
        for i in range(1, HOP):
            for d in (0, 1):
                far(d, i, f).wait_recv()
        far(0, HOP, f).wait_recv()
        spread(FAR + f)
        forward(FAR + f - 1)
        if f == PARTS - 2:
            gathered(HOP - 1)
            gathered(HOP)
            ffn_in(slice(2 * HOP - 3, mid), full)
    for g in range(HOP, -1, -1):
        ffn_out(g)
    far_blocks = slice(mid, NB)
    for f in range(PARTS):
        if f == PARTS - 1:
            forward(FAR + f)
        gathered(FAR + f)
        ffn_in(far_blocks, items[FAR + f][1], f == 0, f == PARTS - 1)

    def begin(g):
        if g >= FAR:
            ffn_out(g)
        for side in sides(g):
            go(opp, g, side)

    def middle(g):
        k = items[g][1]
        for side in (0, 1):
            if side in sides(g):
                b = half(g, side)
                opp(g, side).wait_recv()

                def add(i, carry):
                    ks = pl.ds(pl.multiple_of(k.start + i * kc, kc), kc)
                    PB[2 - side, b, :, ks] = (PB[2 - side, b, :, ks].astype(F32) + OPP[b, :, ks].astype(F32)).astype(BF16)
                    return carry
                lax.fori_loop(0, (k.stop - k.start) // kc, add, 0)
            go(main, g, side)

    def finish(g):
        b, k = items[g]
        for side in (0, 1):
            main(g, side).wait_recv()

        def add(i, carry):
            ks = pl.ds(pl.multiple_of(k.start + i * kc, kc), kc)
            R[b, :, ks] = (PB[0, b, :, ks].astype(F32) + RX[0, b, :, ks].astype(F32)
                           + RX[1, b, :, ks].astype(F32)).astype(BF16)
            return carry
        lax.fori_loop(0, (k.stop - k.start) // kc, add, 0)
        if g >= FAR:
            f = g - FAR
            go(back, 0, HOP, f)
            for i in range(HOP - 1, 0, -1):
                for d in (0, 1):
                    go(back, d, i, f)

    def weigh(lhs, rhs):
        return lax.dot_general(lhs, rhs, (((0,), (0,)), ((), ())), preferred_element_type=F32)

    def give(j):
        for d in ((0, 1) if j > 0 else (0,)):
            o = idx(d, j)
            w_own = own(o, True)
            w_far = None
            if j == HOP:
                w_far = beyond(o, d, True)

            def step(f):
                u = weigh(w_own, R[o, :, cols(f)])
                if j == HOP:
                    for i in range(1, HOP):
                        back(d, i, f).wait_recv()
                    if d == 0:
                        back(0, HOP, f).wait_recv()
                    u = u + weigh(w_far, FR[d, :, :, cols(f)].reshape(HOP * blk, fw))
                C[o, :, cols(f)] = u[:rows].astype(BF16)
                CP[o, :, cols(f)] = u[rows:].astype(BF16)
                p_con(o, f).start()
            each_part(step)
            note(p_con, o)

    def pass_on(j):
        def step(f):
            for d in (0, 1):
                o = idx(d, j)
                p_con(o, f).wait_recv()
                v = C[o, :, cols(f)].astype(F32) + CR[o, :, cols(f)].astype(F32)
                if j < HOP:
                    ring(d, j + 1, f).wait_recv()
                    v = v + RZ[d, j, :, cols(f)].astype(F32)
                C[o, :, cols(f)] = v.astype(BF16)
                ring(d, j, f).start()
        each_part(step)
        note(ring, 0, j)
        note(ring, 1, j)

    far_items = list(range(FAR, FAR + PARTS))
    order = far_items + list(range(HOP, -1, -1))
    begin(order[0])
    for n, g in enumerate(order):
        if n + 1 < len(order):
            begin(order[n + 1])
        middle(g)
        if n >= 2:
            h = order[n - 2]
            finish(h)
            if h < FAR:
                give(h)
            if h == HOP:
                pass_on(h)
            if h + 1 < HOP and h < FAR:
                pass_on(h + 1)
    finish(1)
    give(1)
    pass_on(2)
    finish(0)
    give(0)
    pass_on(1)

    def last(f):
        p_con(0, f).wait_recv()
        ring(0, 1, f).wait_recv()
        ring(1, 1, f).wait_recv()
        out[:, cols(f)] = (C[0, :, cols(f)].astype(F32) + CR[0, :, cols(f)].astype(F32)
                           + RZ[0, 0, :, cols(f)].astype(F32) + RZ[1, 0, :, cols(f)].astype(F32)).astype(BF16)
    each_part(last)

    for make, a, looped in sent:
        if looped:
            each_part(lambda f: make(*a, f).wait_send())
        else:
            make(*a).wait_send()


def on_device(tokens, expert_ids, gate_scores, norm_gain, w_gate, w_up, w_down):
    rows, width = tokens.shape
    E, NX = lax.axis_size("expert"), lax.axis_size("tensor")
    cap = 4 * rows // E
    Z, HOP, blk, hid = E // 2, E // 8, 2 * cap, w_gate.shape[2]
    NG, NO = HOP + 1 + PARTS, 2 * HOP + 1
    v = lambda *s: pltpu.VMEM(s, BF16)
    return pl.pallas_call(
        functools.partial(kernel, E, NX, rows, width),
        out_shape=jax.ShapeDtypeStruct((rows, width), BF16),
        in_specs=[pl.BlockSpec(memory_space=pltpu.VMEM)] * 4 + [pl.BlockSpec(memory_space=pl.ANY)] * 3,
        out_specs=pl.BlockSpec(memory_space=pltpu.VMEM),
        scratch_shapes=[
            v(NO, 2, rows, width),
            pltpu.VMEM((NO, 2, 8, 128), F32),
            v(2, HOP, blk, width),
            v(NX, Z, blk, width),
            v(width, hid), v(width, hid), v(hid, width),
            pltpu.VMEM((2, NX * (Z - NO) * blk, hid), F32),
            v(NX, Z, blk, hid),
            v(NX, Z, blk, width),
            v(Z, blk, width),
            v(2, Z, blk, width),
            v(Z, blk, width),
            v(2, HOP, blk, width),
            v(NO, rows, width), v(NO, rows, width), v(NO, rows, width),
            v(2, HOP, rows, width),
            DMA((3,)),
            DMA((2, HOP, PARTS)), DMA((2, HOP, PARTS)), DMA((NO, PARTS)), DMA((NO, PARTS)),
            DMA((2, HOP)), DMA((2, HOP)), DMA((NO,)), DMA((NO,)),
            DMA((2, HOP, PARTS)), DMA((2, HOP, PARTS)),
            DMA((NG, 2)), DMA((NG, 2)), DMA((NG, 2)), DMA((NG, 2)),
            DMA((NG, 2)), DMA((NG, 2)), DMA((NG, 2)), DMA((NG, 2)),
            DMA((2, HOP, PARTS)), DMA((2, HOP, PARTS)),
            DMA((NO, PARTS)), DMA((NO, PARTS)),
            DMA((2, HOP, PARTS)), DMA((2, HOP, PARTS)),
        ],
        compiler_params=pltpu.CompilerParams(collective_id=0, has_side_effects=True, vmem_limit_bytes=63 * 1024 * 1024),
    )(tokens, expert_ids.T, gate_scores.T, norm_gain.reshape(1, width), w_gate, w_up, w_down)


def solution(mesh):
    return jax.shard_map(
        on_device,
        mesh=mesh,
        in_specs=(
            P(("groups", "expert", "tensor"), None),
            P(("groups", "expert", "tensor"), None),
            P(("groups", "expert", "tensor"), None),
            P(),
            P("expert", None, "tensor"),
            P("expert", None, "tensor"),
            P("expert", "tensor", None),
        ),
        out_specs=P(("groups", "expert", "tensor"), None),
        check_vma=False,
    )
```

```python
import functools

import jax
import jax.numpy as jnp
from jax import lax
from jax.experimental import pallas as pl
from jax.experimental.pallas import tpu as pltpu
from jax.sharding import PartitionSpec as P

MESH = pl.DeviceIdType.MESH
F32, BF16 = jnp.float32, jnp.bfloat16
PARTS = 6
ROUNDS = 2
DMA = pltpu.SemaphoreType.DMA


def kernel(E, NX, rows, width, tokens, ids, scores, gain, wg_in, wu_in, wd_in, out,
           T, M, FS, G, WG, WU, WD, ACC, HID, PB, OPP, RX, R, FR, C, CP, CR, RZ,
           wsem, zs, zr, ps, pr, zms, zmr, pms, pmr, fs, fr, xs, xr, xfs, xfr,
           os_, or_, ms_, mr_, bs, br, cs_, cr_, rs, rr):
    Z = E // 2
    HOP = Z // 4
    cap = 4 * rows // E
    blk = 2 * cap
    fw = width // PARTS
    hid = WG.shape[1]
    e = lax.axis_index("expert")
    x = lax.axis_index("tensor")
    c = lax.rem(e, 2)
    sgn = (1, -1)

    def at_z(k):
        return {"expert": lax.rem(e + 2 * k + 2 * E, E)}

    partner = {"expert": e + 1 - 2 * c}
    side_dev = ({"tensor": lax.rem(x + 1, NX)}, {"tensor": lax.rem(x + NX - 1, NX)})

    def cols(f):
        return pl.ds(pl.multiple_of(f * fw, fw), fw)

    def rcopy(src, dst, s, r, dev):
        return pltpu.make_async_remote_copy(src_ref=src, dst_ref=dst, send_sem=s, recv_sem=r,
                                            device_id=dev, device_id_type=MESH)

    PR = PARTS // ROUNDS
    wr = width // ROUNDS

    def each_part(h, body):
        def step(f, carry):
            body(f)
            return carry
        lax.fori_loop(h * PR, (h + 1) * PR, step, 0)

    def idx(d, j):
        return 0 if j == 0 else 2 * j - 1 + d

    def z_meta(d, j):
        return rcopy(M.at[idx(d, j), 0], M.at[idx(d, j + 1), 0],
                     zms.at[d, j], zmr.at[d, j], at_z(sgn[d]))

    def p_meta(o):
        return rcopy(M.at[o, 0], M.at[o, 1], pms.at[o], pmr.at[o], partner)

    def z_tok(d, j, f):
        return rcopy(T.at[idx(d, j), 0, :, cols(f)], T.at[idx(d, j + 1), 0, :, cols(f)], zs.at[d, j, f], zr.at[d, j, f], at_z(sgn[d]))

    def p_tok(o, f):
        return rcopy(T.at[o, 0, :, cols(f)], T.at[o, 1, :, cols(f)], ps.at[o, f], pr.at[o, f], partner)

    def far(d, i, f):
        if i == HOP:
            return rcopy(FS.at[c, i - 1, :, cols(f)], G.at[0, Z - 1, :, cols(f)],
                         fs.at[0, i - 1, f], fr.at[0, i - 1, f],
                         {"expert": lax.rem(e + 2 * i * (1 - 2 * c) + 2 * E, E)})
        return rcopy(FS.at[d, i - 1, :, cols(f)], G.at[0, idx(d, HOP + i), :, cols(f)],
                     fs.at[d, i - 1, f], fr.at[d, i - 1, f], at_z(sgn[d] * i))

    mid, NB = 2 * HOP + 1, Z
    items = []
    for h in range(ROUNDS):
        items.append((slice(0, 1), slice(h * wr, (h + 1) * wr)))
        items += [(slice(2 * j - 1, 2 * j + 1), slice(h * wr, (h + 1) * wr)) for j in range(1, HOP + 1)]
    FAR = len(items)
    items += [(slice(mid, NB), slice(f * fw, (f + 1) * fw)) for f in range(PARTS)]

    def near(h, j):
        return h * (HOP + 1) + j

    def half(g, side):
        b = items[g][0]
        cut = b.start if b.start == 0 else (b.start + b.stop + 1) // 2
        return slice(b.start, cut) if side == 0 else slice(cut, b.stop)

    def sides(g):
        return [s for s in (0, 1) if half(g, s).stop > half(g, s).start]

    def xsend(g, side):
        b, k = items[g]
        return rcopy(G.at[0, b, :, k], G.at[1 + side, b, :, k], xs.at[g, side], xr.at[g, side], side_dev[side])

    def xfwd(g, side):
        b, k = half(g, side), items[g][1]
        return rcopy(G.at[1 + side, b, :, k], G.at[3, b, :, k], xfs.at[g, side], xfr.at[g, side], side_dev[side])

    def opp(g, side):
        b, k = half(g, side), items[g][1]
        return rcopy(PB.at[3, b, :, k], OPP.at[b, :, k], os_.at[g, side], or_.at[g, side], side_dev[side])

    def main(g, side):
        b, k = items[g]
        return rcopy(PB.at[2 - side, b, :, k], RX.at[side, b, :, k], ms_.at[g, side], mr_.at[g, side], side_dev[side])

    def back(d, i, f):
        if i == HOP:
            return rcopy(R.at[Z - 1, :, cols(f)], FR.at[c, i - 1, :, cols(f)], bs.at[0, i - 1, f], br.at[0, i - 1, f],
                         {"expert": lax.rem(e - 2 * i * (1 - 2 * c) + 2 * E, E)})
        return rcopy(R.at[idx(d, HOP + i), :, cols(f)], FR.at[d, i - 1, :, cols(f)],
                     bs.at[d, i - 1, f], br.at[d, i - 1, f], at_z(-sgn[d] * i))

    def p_con(o, f):
        return rcopy(CP.at[o, :, cols(f)], CR.at[o, :, cols(f)], cs_.at[o, f], cr_.at[o, f], partner)

    def ring(d, j, f):
        return rcopy(C.at[idx(d, j), :, cols(f)], RZ.at[d, j - 1, :, cols(f)],
                     rs.at[d, j - 1, f], rr.at[d, j - 1, f], at_z(-sgn[d]))

    lane = lax.broadcasted_iota(jnp.int32, (1, 128), 1)

    def picks(o, n, first, scored):
        def both(r):
            return jnp.where(lane < rows, M[o, 0, r:r + 1, :], M[o, 1, r:r + 1, :])
        r = lax.broadcasted_iota(jnp.int32, (n * blk, 128), 0)
        ln = lax.broadcasted_iota(jnp.int32, (n * blk, 128), 1)
        ex = first(r // blk)
        ex = jnp.where(ex >= E, ex - E, ex)
        ex = jnp.where(ex < 0, ex + E, ex)
        slot = (cap * ex + lax.rem(r, cap)).astype(F32)
        mine = (lax.rem(r, blk) // cap) == (ln // rows)
        one = jnp.ones((n * blk, 128), F32)
        a, b = (both(2), both(3)) if scored else (one, one)
        val = jnp.where(both(0) == slot, a, 0.0) + jnp.where(both(1) == slot, b, 0.0)
        return jnp.where(mine, val, 0.0)[:, :2 * rows].astype(BF16)

    def own(o, scored):
        return picks(o, 1, lambda i: i + e, scored)

    def beyond(o, d, scored):
        return picks(o, HOP, lambda i: e + 2 * sgn[d] * (i + 1), scored)

    def select(lhs, o, f):
        return jnp.dot(lhs, T[o, :, :, cols(f)].reshape(2 * rows, fw), preferred_element_type=F32)

    kc = fw

    def ffn_in(b, k):
        n = NX * (b.stop - b.start) * blk

        def step(i, carry):
            ks = pl.ds(pl.multiple_of(k.start + i * kc, kc), kc)
            lhs = G[:, b, :, ks].reshape(n, kc)
            for m, W in ((0, WG), (1, WU)):
                got = jnp.dot(lhs, W[ks, :], preferred_element_type=F32)
                ACC[m, :, b] += got.reshape(NX, b.stop - b.start, blk, hid)
            return carry
        lax.fori_loop(0, (k.stop - k.start) // kc, step, 0)

    def ffn_mid(b):
        gate = ACC[0, :, b]
        HID[:, b] = (gate / (1.0 + jnp.exp(-gate)) * ACC[1, :, b]).astype(BF16)

    def ffn_out(g):
        b, k = items[g]
        n = NX * (b.stop - b.start) * blk
        lhs = HID[:, b].reshape(n, hid)

        def step(i, carry):
            ks = pl.ds(pl.multiple_of(k.start + i * kc, kc), kc)
            PB[:, b, :, ks] = jnp.dot(lhs, WD[:, ks], preferred_element_type=F32).astype(BF16).reshape(NX, b.stop - b.start, blk, kc)
            return carry
        lax.fori_loop(0, (k.stop - k.start) // kc, step, 0)

    barrier = pltpu.get_barrier_semaphore()
    peers = [at_z(s * k) for k in range(1, HOP + 1) for s in sgn] + list(side_dev) + [partner]
    for dev in peers:
        pl.semaphore_signal(barrier, inc=1, device_id=dev, device_id_type=MESH)
    weights = [pltpu.make_async_copy(wg_in.at[0], WG, wsem.at[0]),
               pltpu.make_async_copy(wu_in.at[0], WU, wsem.at[1]),
               pltpu.make_async_copy(wd_in.at[0], WD, wsem.at[2])]
    for w in weights:
        w.start()

    row_t = lax.broadcasted_iota(jnp.int32, (rows, rows), 0)
    col_t = lax.broadcasted_iota(jnp.int32, (rows, rows), 1)
    named = [ids[k:k + 1, :].astype(F32) for k in (0, 1)]
    stood = [jnp.sum(jnp.where(row_t == col_t, r, 0.0), axis=1, keepdims=True) for r in named]
    M[0, 0] = jnp.zeros((8, 128), F32)
    for k in (0, 1):
        ahead = [jnp.where((q == named[k]) & (row_t < col_t), 1.0, 0.0) for q in stood]
        M[0, 0, k:k + 1, 0:rows] = named[k] * cap + jnp.sum(ahead[0] + ahead[1], axis=0, keepdims=True)
        M[0, 0, 2 + k:3 + k, 0:rows] = scores[k:k + 1, :]
    once = M[0, 0]
    M[0, 0] = jnp.where(lane < 2 * rows, once + pltpu.roll(once, rows, 1), -1.0)

    total = jnp.zeros((rows, 1), F32)
    for k in range(0, width, kc):
        t = tokens[:, k:k + kc].astype(F32)
        total = total + jnp.sum(t * t, axis=1, keepdims=True)
    scale = lax.rsqrt(total / width + 1e-05)
    for k in range(0, width, kc):
        T[0, 0, :, k:k + kc] = (tokens[:, k:k + kc].astype(F32) * scale * gain[:, k:k + kc]).astype(BF16)
    ACC[...] = jnp.zeros_like(ACC)
    FR[1 - c, HOP - 1] = jnp.zeros((blk, width), BF16)
    pl.semaphore_wait(barrier, len(peers))

    sent = []

    def go(make, *a):
        make(*a).start()
        sent.append((make, a, None))

    def note(h, make, *a):
        sent.append((make, a, h))

    for d in (0, 1):
        go(z_meta, d, 0)
    go(p_meta, 0)

    def launch(h):
        def first(f):
            p_tok(0, f).start()
            z_tok(0, 0, f).start()
            z_tok(1, 0, f).start()
        each_part(h, first)
        note(h, p_tok, 0)
        note(h, z_tok, 0, 0)
        note(h, z_tok, 1, 0)

    def spread(g):
        go(xsend, g, 0)
        go(xsend, g, 1)

    def forward(g):
        for side in (0, 1):
            xsend(g, side).wait_recv()
            if side in sides(g):
                go(xfwd, g, side)

    def gathered(g):
        for side in sides(g):
            xfwd(g, side).wait_recv()

    def own_chip(h):
        lhs = own(0, False)

        def sel(f):
            p_tok(0, f).wait_recv()
            G[0, 0, :, cols(f)] = select(lhs, 0, f).astype(BF16)
        each_part(h, sel)
        spread(near(h, 0))

    def meta_hop(j):
        for d in (0, 1):
            z_meta(d, j - 1).wait_recv()
            if j < HOP:
                go(z_meta, d, j)
            go(p_meta, idx(d, j))

    def hop(h, j):
        def step(f):
            for d in (0, 1):
                z_tok(d, j - 1, f).wait_recv()
                if j < HOP:
                    z_tok(d, j, f).start()
                p_tok(idx(d, j), f).start()
        each_part(h, step)
        for d in (0, 1):
            if j < HOP:
                note(h, z_tok, d, j)
            note(h, p_tok, idx(d, j))

    def choose(h, j):
        lhs = [own(idx(d, j), False) for d in (0, 1)]
        if j == HOP:
            lhs = [jnp.concatenate([lhs[d], beyond(idx(d, j), d, False)], axis=0) for d in (0, 1)]

        def sel(f):
            for d in (0, 1):
                o = idx(d, j)
                p_tok(o, f).wait_recv()
                got = select(lhs[d], o, f).astype(BF16)
                G[0, o, :, cols(f)] = got[:blk]
                if j == HOP:
                    FS[d, :, :, cols(f)] = got[blk:].reshape(HOP, blk, fw)
            if j == HOP:
                for i in range(1, HOP):
                    for d in (0, 1):
                        far(d, i, f).start()
                far(0, HOP, f).start()
        each_part(h, sel)
        if j == HOP:
            for i in range(1, HOP):
                for d in (0, 1):
                    note(h, far, d, i)
            note(h, far, 0, HOP)
        spread(near(h, j))

    def far_in(f):
        for i in range(1, HOP):
            for d in (0, 1):
                far(d, i, f).wait_recv()
        far(0, HOP, f).wait_recv()
        spread(FAR + f)

    nears, fars = slice(0, mid), slice(mid, NB)

    launch(0)
    p_meta(0).wait_recv()
    before = None
    for h in range(ROUNDS):
        own_chip(h)
        if before is not None:
            forward(before)
        before = near(h, 0)
        for j in range(1, HOP + 1):
            if h == 0:
                meta_hop(j)
            hop(h, j)
            if j == HOP and h + 1 < ROUNDS:
                launch(h + 1)
            if h == 0:
                for d in (0, 1):
                    p_meta(idx(d, j)).wait_recv()
            choose(h, j)
            forward(before)
            before = near(h, j)
            if h > 0 and j == 1:
                for f in range((h - 1) * PR, h * PR):
                    far_in(f)
                    forward(before)
                    before = FAR + f
            if h > 0 and j == HOP - 1:
                if h == 1:
                    for w in weights:
                        w.wait()
                for jj in range(HOP + 1):
                    gathered(near(h - 1, jj))
                ffn_in(nears, slice((h - 1) * wr, h * wr))
            if h > 0 and j == HOP:
                for f in range((h - 1) * PR, h * PR):
                    gathered(FAR + f)
                ffn_in(fars, slice((h - 1) * wr, h * wr))
    h = ROUNDS - 1
    for f in range(h * PR, PARTS):
        far_in(f)
        forward(before)
        before = FAR + f
    for j in range(HOP + 1):
        gathered(near(h, j))
    ffn_in(nears, slice(h * wr, width))
    ffn_mid(nears)
    forward(before)
    for j in range(HOP, -1, -1):
        ffn_out(near(0, j))
    for f in range(h * PR, PARTS):
        gathered(FAR + f)
        ffn_in(fars, items[FAR + f][1])
    ffn_mid(fars)

    def begin(g):
        if g > HOP:
            ffn_out(g)
        for side in sides(g):
            go(opp, g, side)

    def middle(g):
        k = items[g][1]
        for side in (0, 1):
            if side in sides(g):
                b = half(g, side)
                opp(g, side).wait_recv()

                def add(i, carry):
                    ks = pl.ds(pl.multiple_of(k.start + i * kc, kc), kc)
                    PB[2 - side, b, :, ks] = (PB[2 - side, b, :, ks].astype(F32) + OPP[b, :, ks].astype(F32)).astype(BF16)
                    return carry
                lax.fori_loop(0, (k.stop - k.start) // kc, add, 0)
            go(main, g, side)

    def finish(g):
        b, k = items[g]
        for side in (0, 1):
            main(g, side).wait_recv()

        def add(i, carry):
            ks = pl.ds(pl.multiple_of(k.start + i * kc, kc), kc)
            R[b, :, ks] = (PB[0, b, :, ks].astype(F32) + RX[0, b, :, ks].astype(F32)
                           + RX[1, b, :, ks].astype(F32)).astype(BF16)
            return carry
        lax.fori_loop(0, (k.stop - k.start) // kc, add, 0)
        if g >= FAR:
            f = g - FAR
            go(back, 0, HOP, f)
            for i in range(HOP - 1, 0, -1):
                for d in (0, 1):
                    go(back, d, i, f)

    def weigh(lhs, rhs):
        return lax.dot_general(lhs, rhs, (((0,), (0,)), ((), ())), preferred_element_type=F32)

    def give(h, j):
        for d in ((0, 1) if j > 0 else (0,)):
            o = idx(d, j)
            w_own = own(o, True)
            w_far = beyond(o, d, True) if j == HOP else None

            def step(f):
                u = weigh(w_own, R[o, :, cols(f)])
                if j == HOP:
                    for i in range(1, HOP):
                        back(d, i, f).wait_recv()
                    if d == 0:
                        back(0, HOP, f).wait_recv()
                    u = u + weigh(w_far, FR[d, :, :, cols(f)].reshape(HOP * blk, fw))
                C[o, :, cols(f)] = u[:rows].astype(BF16)
                CP[o, :, cols(f)] = u[rows:].astype(BF16)
                p_con(o, f).start()
            each_part(h, step)
            note(h, p_con, o)

    def pass_on(h, j):
        def step(f):
            for d in (0, 1):
                o = idx(d, j)
                p_con(o, f).wait_recv()
                v = C[o, :, cols(f)].astype(F32) + CR[o, :, cols(f)].astype(F32)
                if j < HOP:
                    ring(d, j + 1, f).wait_recv()
                    v = v + RZ[d, j, :, cols(f)].astype(F32)
                C[o, :, cols(f)] = v.astype(BF16)
                ring(d, j, f).start()
        each_part(h, step)
        note(h, ring, 0, j)
        note(h, ring, 1, j)

    def last(h):
        def step(f):
            p_con(0, f).wait_recv()
            ring(0, 1, f).wait_recv()
            ring(1, 1, f).wait_recv()
            out[:, cols(f)] = (C[0, :, cols(f)].astype(F32) + CR[0, :, cols(f)].astype(F32)
                               + RZ[0, 0, :, cols(f)].astype(F32) + RZ[1, 0, :, cols(f)].astype(F32)).astype(BF16)
        each_part(h, step)

    order = []
    for h in range(ROUNDS):
        order += [(FAR + f, h, None) for f in range(h * PR, (h + 1) * PR)]
        order += [(near(h, j), h, j) for j in range(HOP, -1, -1)]
    lag = 2
    todo = {}
    for n, (g, h, j) in enumerate(order):
        if j == HOP:
            for k in range(HOP, -1, -1):
                todo.setdefault(n + lag * (HOP - k), []).append((h, k))
    begin(order[0][0])
    begin(order[1][0])
    steps = max(len(order) + 2, max(todo) + 3)
    for n in range(steps):
        if n + 2 < len(order):
            begin(order[n + 2][0])
        if n < len(order):
            middle(order[n][0])
        if 0 <= n - 2 < len(order):
            g, h, j = order[n - 2]
            finish(g)
            if j is not None:
                give(h, j)
        for h, k in todo.get(n - 2, ()):
            if k > 0:
                pass_on(h, k)
            else:
                last(h)

    for make, a, h in sent:
        if h is None:
            make(*a).wait_send()
        else:
            each_part(h, lambda f: make(*a, f).wait_send())


def on_device(tokens, expert_ids, gate_scores, norm_gain, w_gate, w_up, w_down):
    rows, width = tokens.shape
    E, NX = lax.axis_size("expert"), lax.axis_size("tensor")
    cap = 4 * rows // E
    Z, HOP, blk, hid = E // 2, E // 8, 2 * cap, w_gate.shape[2]
    NG, NO = ROUNDS * (HOP + 1) + PARTS, 2 * HOP + 1
    v = lambda *s: pltpu.VMEM(s, BF16)
    return pl.pallas_call(
        functools.partial(kernel, E, NX, rows, width),
        out_shape=jax.ShapeDtypeStruct((rows, width), BF16),
        in_specs=[pl.BlockSpec(memory_space=pltpu.VMEM)] * 4 + [pl.BlockSpec(memory_space=pl.ANY)] * 3,
        out_specs=pl.BlockSpec(memory_space=pltpu.VMEM),
        scratch_shapes=[
            v(NO, 2, rows, width),
            pltpu.VMEM((NO, 2, 8, 128), F32),
            v(2, HOP, blk, width),
            v(NX, Z, blk, width),
            v(width, hid), v(width, hid), v(hid, width),
            pltpu.VMEM((2, NX, Z, blk, hid), F32),
            v(NX, Z, blk, hid),
            v(NX, Z, blk, width),
            v(Z, blk, width),
            v(2, Z, blk, width),
            v(Z, blk, width),
            v(2, HOP, blk, width),
            v(NO, rows, width), v(NO, rows, width), v(NO, rows, width),
            v(2, HOP, rows, width),
            DMA((3,)),
            DMA((2, HOP, PARTS)), DMA((2, HOP, PARTS)), DMA((NO, PARTS)), DMA((NO, PARTS)),
            DMA((2, HOP)), DMA((2, HOP)), DMA((NO,)), DMA((NO,)),
            DMA((2, HOP, PARTS)), DMA((2, HOP, PARTS)),
            DMA((NG, 2)), DMA((NG, 2)), DMA((NG, 2)), DMA((NG, 2)),
            DMA((NG, 2)), DMA((NG, 2)), DMA((NG, 2)), DMA((NG, 2)),
            DMA((2, HOP, PARTS)), DMA((2, HOP, PARTS)),
            DMA((NO, PARTS)), DMA((NO, PARTS)),
            DMA((2, HOP, PARTS)), DMA((2, HOP, PARTS)),
        ],
        compiler_params=pltpu.CompilerParams(collective_id=0, has_side_effects=True, vmem_limit_bytes=63 * 1024 * 1024),
    )(tokens, expert_ids.T, gate_scores.T, norm_gain.reshape(1, width), w_gate, w_up, w_down)


def solution(mesh):
    return jax.shard_map(
        on_device,
        mesh=mesh,
        in_specs=(
            P(("groups", "expert", "tensor"), None),
            P(("groups", "expert", "tensor"), None),
            P(("groups", "expert", "tensor"), None),
            P(),
            P("expert", None, "tensor"),
            P("expert", None, "tensor"),
            P("expert", "tensor", None),
        ),
        out_specs=P(("groups", "expert", "tensor"), None),
        check_vma=False,
    )
```

```python
import functools

import jax
import jax.numpy as jnp
from jax import lax
from jax.experimental import pallas as pl
from jax.experimental.pallas import tpu as pltpu
from jax.sharding import PartitionSpec as P

MESH = pl.DeviceIdType.MESH
F32, BF16 = jnp.float32, jnp.bfloat16
PARTS = 4
DMA = pltpu.SemaphoreType.DMA
ORDER = [
    ("L", 0), ("L", 1), ("S", 0, 0), ("L", 2), ("S", 0, 1), ("S", 0, 2), ("L", 3), ("H", 1, 0), ("S", 0, 3),
    ("S", 1, 0), ("X", 0, 0), ("H", 1, 1), ("S", 1, 1), ("X", 0, 1), ("H", 1, 2), ("XF", 0, 0), ("S", 1, 2),
    ("X", 0, 2), ("H", 1, 3), ("XF", 0, 1), ("S", 1, 3), ("X", 0, 3), ("H", 2, 0), ("S", 2, 0), ("XF", 0, 2),
    ("H", 2, 1), ("S", 2, 1), ("XF", 0, 3), ("H", 2, 2), ("S", 2, 2), ("H", 2, 3), ("S", 2, 3), ("H", 3, 0),
    ("S", 3, 0), ("X", 1, 0), ("H", 3, 1), ("S", 3, 1), ("X", 1, 1), ("H", 3, 2), ("S", 3, 2), ("X", 1, 2),
    ("XF", 1, 0), ("H", 3, 3), ("S", 3, 3), ("X", 1, 3), ("XF", 1, 1), ("H", 4, 0), ("S", 4, 0), ("X", 2, 0),
    ("XF", 1, 2), ("H", 4, 1), ("S", 4, 1), ("X", 2, 1), ("H", 4, 2), ("XF", 1, 3), ("S", 4, 2), ("X", 2, 2),
    ("H", 4, 3), ("XF", 2, 0), ("S", 4, 3), ("X", 2, 3), ("XF", 2, 1), ("XF", 2, 2), ("FI", 0, 0), ("X", 3, 0),
    ("XF", 2, 3), ("FI", 0, 1), ("FI", 0, 2), ("X", 3, 1), ("XF", 3, 0), ("FI", 0, 3), ("FM", 0), ("FO", 0, 0),
    ("FO", 0, 1), ("X", 3, 2), ("FO", 0, 2), ("FO", 0, 3), ("XF", 3, 1), ("FI", 1, 0), ("X", 3, 3), ("XF", 3, 2),
    ("FI", 1, 1), ("O", 2, 0), ("O", 1, 0), ("XF", 3, 3), ("FI", 1, 2), ("O", 0, 0), ("M", 2, 0), ("M", 1, 0),
    ("FI", 1, 3), ("FM", 1), ("M", 0, 0), ("FO", 1, 0), ("FO", 1, 1), ("N", 2, 0), ("FO", 1, 2), ("FO", 1, 3),
    ("O", 3, 0), ("N", 1, 0), ("G", 3, 0), ("G", 2, 0), ("O", 3, 1), ("N", 0, 0), ("G", 1, 0), ("G", 0, 0),
    ("O", 3, 2), ("M", 3, 0), ("M", 3, 1), ("M", 3, 2), ("N", 3, 0), ("N", 3, 1), ("O", 2, 1), ("O", 1, 1),
    ("O", 0, 1), ("O", 3, 3), ("G", 4, 0), ("N", 3, 2), ("M", 2, 1), ("P", 4, 0), ("M", 1, 1), ("M", 0, 1),
    ("M", 3, 3), ("N", 2, 1), ("G", 4, 1), ("P", 4, 1), ("N", 1, 1), ("G", 3, 1), ("G", 2, 1), ("N", 0, 1),
    ("G", 1, 1), ("G", 0, 1), ("O", 2, 2), ("P", 3, 0), ("O", 1, 2), ("O", 0, 2), ("O", 2, 3), ("P", 3, 1),
    ("O", 1, 3), ("N", 3, 3), ("M", 2, 2), ("M", 1, 2), ("P", 2, 0), ("M", 0, 2), ("M", 2, 3), ("P", 2, 1),
    ("M", 1, 3), ("N", 2, 2), ("G", 4, 2), ("P", 4, 2), ("N", 1, 2), ("G", 3, 2), ("G", 2, 2), ("O", 0, 3),
    ("N", 0, 2), ("G", 1, 2), ("G", 0, 2), ("N", 2, 3), ("G", 4, 3), ("P", 1, 0), ("P", 4, 3), ("N", 1, 3),
    ("G", 3, 3), ("P", 1, 1), ("G", 2, 3), ("M", 0, 3), ("P", 3, 2), ("E", 0), ("N", 0, 3), ("G", 1, 3), ("G", 0, 3),
    ("P", 3, 3), ("E", 1), ("P", 2, 2), ("P", 2, 3), ("P", 1, 2), ("P", 1, 3), ("E", 2), ("E", 3),
]


def kernel(E, NX, rows, width, tokens, ids, scores, gain, wg_in, wu_in, wd_in, out,
           T, M, FS, G, WG, WU, WD, ACC, HID, PB, OPP, RX, R, FR, C, CP, CR, RZ,
           wsem, zs, zr, ps, pr, zms, zmr, pms, pmr, fs, fr, xs, xr, xfs, xfr,
           os_, or_, ms_, mr_, bs, br, cs_, cr_, rs, rr):
    Z = E // 2
    HOP = Z // 4
    cap = 4 * rows // E
    blk = 2 * cap
    fw = width // PARTS
    hid = WG.shape[1]
    e = lax.axis_index("expert")
    x = lax.axis_index("tensor")
    c = lax.rem(e, 2)
    sgn = (1, -1)

    def at_z(k):
        return {"expert": lax.rem(e + 2 * k + 2 * E, E)}

    partner = {"expert": e + 1 - 2 * c}
    side_dev = ({"tensor": lax.rem(x + 1, NX)}, {"tensor": lax.rem(x + NX - 1, NX)})

    def cols(f):
        return slice(f * fw, (f + 1) * fw)

    def rcopy(src, dst, s, r, dev):
        return pltpu.make_async_remote_copy(src_ref=src, dst_ref=dst, send_sem=s, recv_sem=r,
                                            device_id=dev, device_id_type=MESH)

    def idx(d, j):
        return 0 if j == 0 else 2 * j - 1 + d

    def z_meta(d, j):
        return rcopy(M.at[idx(d, j), 0], M.at[idx(d, j + 1), 0],
                     zms.at[d, j], zmr.at[d, j], at_z(sgn[d]))

    def p_meta(o):
        return rcopy(M.at[o, 0], M.at[o, 1], pms.at[o], pmr.at[o], partner)

    def z_tok(d, j, f):
        return rcopy(T.at[idx(d, j), 0, :, cols(f)], T.at[idx(d, j + 1), 0, :, cols(f)], zs.at[d, j, f], zr.at[d, j, f], at_z(sgn[d]))

    def p_tok(o, f):
        return rcopy(T.at[o, 0, :, cols(f)], T.at[o, 1, :, cols(f)], ps.at[o, f], pr.at[o, f], partner)

    def far(d, i, f):
        if i == HOP:
            return rcopy(FS.at[c, i - 1, :, cols(f)], G.at[0, Z - 1, :, cols(f)],
                         fs.at[0, i - 1, f], fr.at[0, i - 1, f],
                         {"expert": lax.rem(e + 2 * i * (1 - 2 * c) + 2 * E, E)})
        return rcopy(FS.at[d, i - 1, :, cols(f)], G.at[0, idx(d, HOP + i), :, cols(f)],
                     fs.at[d, i - 1, f], fr.at[d, i - 1, f], at_z(sgn[d] * i))

    mid, NB = 2 * HOP + 1, Z
    groups = [(0, 3), (3, 2 * HOP - 1), (2 * HOP - 1, mid), (mid, NB)]
    FARG = len(groups) - 1
    nears, fars = slice(0, mid), slice(mid, NB)

    def half(g, side):
        b0, b1 = groups[g]
        cut = (b0 + b1 + (g == FARG)) // 2
        return slice(b0, cut) if side == 0 else slice(cut, b1)

    def xsend(g, f, side):
        b, k, n = slice(*groups[g]), cols(f), g * PARTS + f
        return rcopy(G.at[0, b, :, k], G.at[1 + side, b, :, k], xs.at[n, side], xr.at[n, side], side_dev[side])

    def xfwd(g, f, side):
        b, k, n = half(g, side), cols(f), g * PARTS + f
        return rcopy(G.at[1 + side, b, :, k], G.at[3, b, :, k], xfs.at[n, side], xfr.at[n, side], side_dev[side])

    def opp(g, f, side):
        b, k, n = half(g, side), cols(f), g * PARTS + f
        return rcopy(PB.at[3, b, :, k], OPP.at[b, :, k], os_.at[n, side], or_.at[n, side], side_dev[side])

    def main(g, f, side):
        b, k, n = slice(*groups[g]), cols(f), g * PARTS + f
        return rcopy(PB.at[2 - side, b, :, k], RX.at[side, b, :, k], ms_.at[n, side], mr_.at[n, side], side_dev[side])

    def back(d, i, f):
        if i == HOP:
            return rcopy(R.at[Z - 1, :, cols(f)], FR.at[c, i - 1, :, cols(f)], bs.at[0, i - 1, f], br.at[0, i - 1, f],
                         {"expert": lax.rem(e - 2 * i * (1 - 2 * c) + 2 * E, E)})
        return rcopy(R.at[idx(d, HOP + i), :, cols(f)], FR.at[d, i - 1, :, cols(f)],
                     bs.at[d, i - 1, f], br.at[d, i - 1, f], at_z(-sgn[d] * i))

    def p_con(o, f):
        return rcopy(CP.at[o, :, cols(f)], CR.at[o, :, cols(f)], cs_.at[o, f], cr_.at[o, f], partner)

    def ring(d, j, f):
        return rcopy(C.at[idx(d, j), :, cols(f)], RZ.at[d, j - 1, :, cols(f)],
                     rs.at[d, j - 1, f], rr.at[d, j - 1, f], at_z(-sgn[d]))

    lane = lax.broadcasted_iota(jnp.int32, (1, 128), 1)

    def picks(o, n, first, scored):
        def both(r):
            return jnp.where(lane < rows, M[o, 0, r:r + 1, :], M[o, 1, r:r + 1, :])
        r = lax.broadcasted_iota(jnp.int32, (n * blk, 128), 0)
        ln = lax.broadcasted_iota(jnp.int32, (n * blk, 128), 1)
        ex = first(r // blk)
        ex = jnp.where(ex >= E, ex - E, ex)
        ex = jnp.where(ex < 0, ex + E, ex)
        slot = (cap * ex + lax.rem(r, cap)).astype(F32)
        mine = (lax.rem(r, blk) // cap) == (ln // rows)
        one = jnp.ones((n * blk, 128), F32)
        a, b = (both(2), both(3)) if scored else (one, one)
        val = jnp.where(both(0) == slot, a, 0.0) + jnp.where(both(1) == slot, b, 0.0)
        return jnp.where(mine, val, 0.0)[:, :2 * rows].astype(BF16)

    def own(o, scored):
        return picks(o, 1, lambda i: i + e, scored)

    def beyond(o, d, scored):
        return picks(o, HOP, lambda i: e + 2 * sgn[d] * (i + 1), scored)

    def select(lhs, o, f):
        return jnp.dot(lhs, T[o, :, :, cols(f)].reshape(2 * rows, fw), preferred_element_type=F32)

    kc = fw

    def ffn_in(b, f):
        n = NX * (b.stop - b.start) * blk
        lhs = G[:, b, :, cols(f)].reshape(n, fw)
        for m, W in ((0, WG), (1, WU)):
            got = jnp.dot(lhs, W[cols(f), :], preferred_element_type=F32)
            ACC[m, :, b] += got.reshape(NX, b.stop - b.start, blk, hid)

    def ffn_mid(b):
        gate = ACC[0, :, b]
        HID[:, b] = (gate / (1.0 + jnp.exp(-gate)) * ACC[1, :, b]).astype(BF16)

    def ffn_out(b, f):
        n = NX * (b.stop - b.start) * blk
        got = jnp.dot(HID[:, b].reshape(n, hid), WD[:, cols(f)], preferred_element_type=F32)
        PB[:, b, :, cols(f)] = got.astype(BF16).reshape(NX, b.stop - b.start, blk, fw)

    barrier = pltpu.get_barrier_semaphore()
    peers = [at_z(s * k) for k in range(1, HOP + 1) for s in sgn] + list(side_dev) + [partner]
    for dev in peers:
        pl.semaphore_signal(barrier, inc=1, device_id=dev, device_id_type=MESH)
    weights = [pltpu.make_async_copy(wg_in.at[0], WG, wsem.at[0]),
               pltpu.make_async_copy(wu_in.at[0], WU, wsem.at[1]),
               pltpu.make_async_copy(wd_in.at[0], WD, wsem.at[2])]
    for w in weights:
        w.start()

    row_t = lax.broadcasted_iota(jnp.int32, (rows, rows), 0)
    col_t = lax.broadcasted_iota(jnp.int32, (rows, rows), 1)
    named = [ids[k:k + 1, :].astype(F32) for k in (0, 1)]
    stood = [jnp.sum(jnp.where(row_t == col_t, r, 0.0), axis=1, keepdims=True) for r in named]
    M[0, 0] = jnp.zeros((8, 128), F32)
    for k in (0, 1):
        ahead = [jnp.where((q == named[k]) & (row_t < col_t), 1.0, 0.0) for q in stood]
        M[0, 0, k:k + 1, 0:rows] = named[k] * cap + jnp.sum(ahead[0] + ahead[1], axis=0, keepdims=True)
        M[0, 0, 2 + k:3 + k, 0:rows] = scores[k:k + 1, :]
    once = M[0, 0]
    M[0, 0] = jnp.where(lane < 2 * rows, once + pltpu.roll(once, rows, 1), -1.0)

    total = jnp.zeros((rows, 1), F32)
    for k in range(0, width, kc):
        t = tokens[:, k:k + kc].astype(F32)
        total = total + jnp.sum(t * t, axis=1, keepdims=True)
    scale = lax.rsqrt(total / width + 1e-05)
    for k in range(0, width, kc):
        T[0, 0, :, k:k + kc] = (tokens[:, k:k + kc].astype(F32) * scale * gain[:, k:k + kc]).astype(BF16)
    ACC[...] = jnp.zeros_like(ACC)
    FR[1 - c, HOP - 1] = jnp.zeros((blk, width), BF16)
    pl.semaphore_wait(barrier, len(peers))

    sent = []

    def go(make, *a):
        make(*a).start()
        sent.append((make, a))

    def weigh(lhs, rhs):
        return lax.dot_general(lhs, rhs, (((0,), (0,)), ((), ())), preferred_element_type=F32)

    seen = set()

    def new(*key):
        fresh = key not in seen
        seen.add(key)
        return fresh

    def launch(f):
        go(p_tok, 0, f)
        go(z_tok, 0, 0, f)
        go(z_tok, 1, 0, f)

    def hop(j, f):
        if new("hop", j):
            for d in (0, 1):
                z_meta(d, j - 1).wait_recv()
                if j < HOP:
                    go(z_meta, d, j)
                go(p_meta, idx(d, j))
        for d in (0, 1):
            z_tok(d, j - 1, f).wait_recv()
            if j < HOP:
                go(z_tok, d, j, f)
            go(p_tok, idx(d, j), f)

    def choose(j, f):
        for d in ((0, 1) if j > 0 else (0,)):
            o = idx(d, j)
            if new("choose", o):
                p_meta(o).wait_recv()
            lhs = own(o, False)
            if j == HOP:
                lhs = jnp.concatenate([lhs, beyond(o, d, False)], axis=0)
            p_tok(o, f).wait_recv()
            got = select(lhs, o, f).astype(BF16)
            G[0, o, :, cols(f)] = got[:blk]
            if j == HOP:
                FS[d, :, :, cols(f)] = got[blk:].reshape(HOP, blk, fw)
        if j == HOP:
            for i in range(1, HOP):
                for d in (0, 1):
                    go(far, d, i, f)
            go(far, 0, HOP, f)

    def spread(g, f):
        if g == FARG:
            for i in range(1, HOP):
                for d in (0, 1):
                    far(d, i, f).wait_recv()
            far(0, HOP, f).wait_recv()
        for side in (0, 1):
            go(xsend, g, f, side)

    def forward(g, f):
        for side in (0, 1):
            xsend(g, f, side).wait_recv()
            go(xfwd, g, f, side)

    def layer_in(q, f):
        if new("weights"):
            for w in weights:
                w.wait()
        for g in (range(FARG) if q == 0 else (FARG,)):
            for side in (0, 1):
                xfwd(g, f, side).wait_recv()
        ffn_in((nears, fars)[q], f)

    def layer_mid(q):
        ffn_mid((nears, fars)[q])

    def layer_out(q, f):
        ffn_out((nears, fars)[q], f)

    def begin(g, f):
        for side in (0, 1):
            go(opp, g, f, side)

    def middle(g, f):
        k = cols(f)
        for side in (0, 1):
            b = half(g, side)
            opp(g, f, side).wait_recv()
            PB[2 - side, b, :, k] = (PB[2 - side, b, :, k].astype(F32) + OPP[b, :, k].astype(F32)).astype(BF16)
            go(main, g, f, side)

    def finish(g, f):
        b, k = slice(*groups[g]), cols(f)
        for side in (0, 1):
            main(g, f, side).wait_recv()
        R[b, :, k] = (PB[0, b, :, k].astype(F32) + RX[0, b, :, k].astype(F32) + RX[1, b, :, k].astype(F32)).astype(BF16)
        if g == FARG:
            go(back, 0, HOP, f)
            for i in range(HOP - 1, 0, -1):
                for d in (0, 1):
                    go(back, d, i, f)

    def give(j, f):
        for d in ((0, 1) if j > 0 else (0,)):
            o = idx(d, j)
            u = weigh(own(o, True), R[o, :, cols(f)])
            if j == HOP:
                for i in range(1, HOP):
                    back(d, i, f).wait_recv()
                if d == 0:
                    back(0, HOP, f).wait_recv()
                u = u + weigh(beyond(o, d, True), FR[d, :, :, cols(f)].reshape(HOP * blk, fw))
            C[o, :, cols(f)] = u[:rows].astype(BF16)
            CP[o, :, cols(f)] = u[rows:].astype(BF16)
            go(p_con, o, f)

    def pass_on(j, f):
        for d in (0, 1):
            o = idx(d, j)
            p_con(o, f).wait_recv()
            v = C[o, :, cols(f)].astype(F32) + CR[o, :, cols(f)].astype(F32)
            if j < HOP:
                ring(d, j + 1, f).wait_recv()
                v = v + RZ[d, j, :, cols(f)].astype(F32)
            C[o, :, cols(f)] = v.astype(BF16)
            go(ring, d, j, f)

    def last(f):
        p_con(0, f).wait_recv()
        ring(0, 1, f).wait_recv()
        ring(1, 1, f).wait_recv()
        out[:, cols(f)] = (C[0, :, cols(f)].astype(F32) + CR[0, :, cols(f)].astype(F32)
                           + RZ[0, 0, :, cols(f)].astype(F32) + RZ[1, 0, :, cols(f)].astype(F32)).astype(BF16)

    for d in (0, 1):
        go(z_meta, d, 0)
    go(p_meta, 0)
    run = {"L": launch, "H": hop, "S": choose, "X": spread, "XF": forward, "FI": layer_in, "FM": layer_mid,
           "FO": layer_out, "O": begin, "M": middle, "N": finish, "G": give, "P": pass_on, "E": last}
    for task in ORDER:
        with jax.named_scope("_".join(map(str, task))):
            run[task[0]](*task[1:])
    for make, a in sent:
        make(*a).wait_send()


def on_device(tokens, expert_ids, gate_scores, norm_gain, w_gate, w_up, w_down):
    rows, width = tokens.shape
    E, NX = lax.axis_size("expert"), lax.axis_size("tensor")
    cap = 4 * rows // E
    Z, HOP, blk, hid = E // 2, E // 8, 2 * cap, w_gate.shape[2]
    NG, NO = 4 * PARTS, 2 * HOP + 1
    v = lambda *s: pltpu.VMEM(s, BF16)
    return pl.pallas_call(
        functools.partial(kernel, E, NX, rows, width),
        out_shape=jax.ShapeDtypeStruct((rows, width), BF16),
        in_specs=[pl.BlockSpec(memory_space=pltpu.VMEM)] * 4 + [pl.BlockSpec(memory_space=pl.ANY)] * 3,
        out_specs=pl.BlockSpec(memory_space=pltpu.VMEM),
        scratch_shapes=[
            v(NO, 2, rows, width),
            pltpu.VMEM((NO, 2, 8, 128), F32),
            v(2, HOP, blk, width),
            v(NX, Z, blk, width),
            v(width, hid), v(width, hid), v(hid, width),
            pltpu.VMEM((2, NX, Z, blk, hid), F32),
            v(NX, Z, blk, hid),
            v(NX, Z, blk, width),
            v(Z, blk, width),
            v(2, Z, blk, width),
            v(Z, blk, width),
            v(2, HOP, blk, width),
            v(NO, rows, width), v(NO, rows, width), v(NO, rows, width),
            v(2, HOP, rows, width),
            DMA((3,)),
            DMA((2, HOP, PARTS)), DMA((2, HOP, PARTS)), DMA((NO, PARTS)), DMA((NO, PARTS)),
            DMA((2, HOP)), DMA((2, HOP)), DMA((NO,)), DMA((NO,)),
            DMA((2, HOP, PARTS)), DMA((2, HOP, PARTS)),
            DMA((NG, 2)), DMA((NG, 2)), DMA((NG, 2)), DMA((NG, 2)),
            DMA((NG, 2)), DMA((NG, 2)), DMA((NG, 2)), DMA((NG, 2)),
            DMA((2, HOP, PARTS)), DMA((2, HOP, PARTS)),
            DMA((NO, PARTS)), DMA((NO, PARTS)),
            DMA((2, HOP, PARTS)), DMA((2, HOP, PARTS)),
        ],
        compiler_params=pltpu.CompilerParams(collective_id=0, has_side_effects=True, vmem_limit_bytes=63 * 1024 * 1024),
    )(tokens, expert_ids.T, gate_scores.T, norm_gain.reshape(1, width), w_gate, w_up, w_down)


def solution(mesh):
    return jax.shard_map(
        on_device,
        mesh=mesh,
        in_specs=(
            P(("groups", "expert", "tensor"), None),
            P(("groups", "expert", "tensor"), None),
            P(("groups", "expert", "tensor"), None),
            P(),
            P("expert", None, "tensor"),
            P("expert", None, "tensor"),
            P("expert", "tensor", None),
        ),
        out_specs=P(("groups", "expert", "tensor"), None),
        check_vma=False,
    )
```

```python
import functools

import jax
import jax.numpy as jnp
from jax import lax
from jax.experimental import pallas as pl
from jax.experimental.pallas import tpu as pltpu
from jax.sharding import PartitionSpec as P

MESH = pl.DeviceIdType.MESH
F32, BF16 = jnp.float32, jnp.bfloat16
SHARES = (10, 10, 10, 8, 6, 4)
PARTS = len(SHARES)
GROUPS = ((0, 3), (3, 7), (7, 9), (9, 13), (13, 16))
DMA = pltpu.SemaphoreType.DMA
ORDER = [
    ("L", 1), ("L", 3), ("S", 0, 1), ("S", 0, 3), ("L", 0), ("S", 0, 0), ("H", 1, 1), ("S", 1, 1), ("H", 1, 3),
    ("X", 0, 1), ("S", 1, 3), ("X", 0, 3), ("H", 1, 0), ("S", 1, 0), ("X", 0, 0), ("H", 2, 1), ("XF", 0, 1),
    ("S", 2, 1), ("H", 2, 3), ("XF", 0, 3), ("S", 2, 3), ("H", 2, 0), ("XF", 0, 0), ("S", 2, 0), ("H", 3, 1),
    ("S", 3, 1), ("H", 3, 3), ("X", 1, 1), ("S", 3, 3), ("X", 1, 3), ("H", 3, 0), ("S", 3, 0), ("X", 1, 0),
    ("H", 4, 1), ("L", 4), ("XF", 1, 1), ("L", 2), ("S", 4, 1), ("H", 4, 3), ("S", 0, 4), ("X", 2, 1), ("XF", 1, 3),
    ("S", 0, 2), ("S", 4, 3), ("H", 4, 0), ("X", 2, 3), ("XF", 1, 0), ("H", 1, 4), ("S", 4, 0), ("X", 2, 0),
    ("S", 1, 4), ("X", 0, 4), ("XF", 2, 1), ("H", 1, 2), ("XF", 2, 3), ("S", 1, 2), ("X", 0, 2), ("X", 3, 1),
    ("XF", 2, 0), ("XF", 0, 4), ("FI", 0, 1), ("FI", 0, 3), ("X", 3, 3), ("X", 4, 1), ("XF", 0, 2), ("H", 2, 4),
    ("XF", 3, 1), ("FI", 0, 0), ("X", 4, 3), ("S", 2, 4), ("X", 3, 0), ("XF", 3, 3), ("L", 5), ("XF", 4, 1),
    ("S", 0, 5), ("H", 2, 2), ("X", 4, 0), ("H", 3, 4), ("XF", 4, 3), ("S", 2, 2), ("H", 1, 5), ("S", 3, 4),
    ("X", 1, 4), ("XF", 3, 0), ("S", 1, 5), ("X", 0, 5), ("H", 3, 2), ("FI", 1, 1), ("H", 4, 4), ("S", 3, 2),
    ("XF", 4, 0), ("X", 1, 2), ("H", 2, 5), ("FI", 1, 3), ("S", 4, 4), ("X", 2, 4), ("S", 2, 5), ("XF", 1, 4),
    ("H", 4, 2), ("XF", 0, 5), ("H", 3, 5), ("FI", 1, 0), ("S", 4, 2), ("X", 2, 2), ("S", 3, 5), ("X", 1, 5),
    ("X", 3, 4), ("XF", 1, 2), ("XF", 2, 4), ("H", 4, 5), ("X", 4, 4), ("XF", 2, 2), ("S", 4, 5), ("X", 2, 5),
    ("XF", 1, 5), ("X", 3, 2), ("XF", 3, 4), ("FI", 0, 4), ("XF", 4, 4), ("X", 3, 5), ("FI", 0, 2), ("XF", 2, 5),
    ("X", 4, 2), ("X", 4, 5), ("XF", 3, 2), ("FI", 1, 4), ("XF", 3, 5), ("FI", 0, 5), ("FM", 0), ("FO", 0, 0),
    ("O", 2, 0), ("FO", 0, 1), ("O", 2, 1), ("FO", 0, 2), ("XF", 4, 2), ("FO", 0, 3), ("FO", 0, 4), ("XF", 4, 5),
    ("FO", 0, 5), ("O", 2, 4), ("O", 1, 0), ("M", 2, 0), ("M", 2, 1), ("FI", 1, 2), ("FI", 1, 5), ("FM", 1),
    ("M", 2, 4), ("FO", 1, 0), ("FO", 1, 1), ("O", 4, 0), ("FO", 1, 2), ("M", 1, 0), ("FO", 1, 3), ("FO", 1, 4),
    ("FO", 1, 5), ("N", 2, 0), ("N", 2, 1), ("O", 3, 0), ("N", 2, 4), ("M", 4, 0), ("O", 4, 3), ("N", 1, 0),
    ("G", 3, 0), ("O", 4, 1), ("G", 2, 0), ("M", 3, 0), ("N", 4, 0), ("O", 3, 1), ("M", 4, 3), ("M", 4, 1),
    ("N", 3, 0), ("O", 3, 2), ("M", 3, 1), ("N", 4, 3), ("N", 4, 1), ("O", 3, 4), ("O", 3, 3), ("G", 4, 0),
    ("M", 3, 2), ("P", 4, 0), ("N", 3, 1), ("O", 4, 2), ("M", 3, 4), ("M", 3, 3), ("N", 3, 2), ("O", 4, 5),
    ("M", 4, 2), ("P", 3, 0), ("N", 3, 4), ("O", 4, 4), ("O", 3, 5), ("G", 4, 1), ("N", 3, 3), ("O", 2, 3),
    ("M", 4, 5), ("O", 1, 1), ("P", 4, 1), ("N", 4, 2), ("O", 2, 2), ("M", 4, 4), ("M", 3, 5), ("P", 2, 0),
    ("M", 2, 3), ("N", 4, 5), ("M", 1, 1), ("M", 2, 2), ("N", 4, 4), ("N", 3, 5), ("N", 2, 3), ("G", 4, 3),
    ("O", 2, 5), ("O", 1, 4), ("O", 0, 0), ("O", 1, 5), ("P", 4, 3), ("N", 1, 1), ("G", 2, 1), ("G", 3, 1),
    ("O", 1, 2), ("N", 2, 2), ("G", 4, 2), ("M", 2, 5), ("O", 1, 3), ("M", 1, 4), ("P", 3, 1), ("M", 0, 0),
    ("M", 1, 5), ("P", 4, 2), ("M", 1, 2), ("N", 2, 5), ("G", 4, 5), ("M", 1, 3), ("G", 4, 4), ("P", 4, 5),
    ("N", 1, 4), ("G", 3, 4), ("G", 2, 4), ("P", 4, 4), ("N", 0, 0), ("G", 1, 0), ("P", 2, 1), ("G", 0, 0),
    ("N", 1, 5), ("G", 3, 5), ("G", 2, 5), ("O", 0, 4), ("P", 1, 0), ("O", 0, 5), ("O", 0, 2), ("N", 1, 2),
    ("P", 3, 5), ("G", 3, 2), ("G", 2, 2), ("O", 0, 1), ("P", 3, 4), ("O", 0, 3), ("N", 1, 3), ("G", 2, 3),
    ("P", 3, 2), ("G", 3, 3), ("M", 0, 4), ("M", 0, 5), ("M", 0, 2), ("P", 3, 3), ("M", 0, 1), ("M", 0, 3), ("E", 0),
    ("N", 0, 4), ("G", 1, 4), ("G", 0, 4), ("P", 2, 5), ("N", 0, 5), ("G", 0, 5), ("G", 1, 5), ("P", 2, 4),
    ("N", 0, 2), ("G", 0, 2), ("G", 1, 2), ("P", 2, 2), ("N", 0, 1), ("G", 1, 1), ("G", 0, 1), ("N", 0, 3),
    ("G", 0, 3), ("G", 1, 3), ("P", 2, 3), ("P", 1, 1), ("P", 1, 5), ("P", 1, 4), ("P", 1, 2), ("P", 1, 3), ("E", 1),
    ("E", 5), ("E", 4), ("E", 2), ("E", 3),
]


def kernel(E, NX, rows, width, tokens, ids, scores, gain, wg_in, wu_in, wd_in, out,
           T, M, FS, G, WG, WU, WD, ACC, HID, PB, OPP, RX, R, FR, C, CP, CR, RZ,
           wsem, zs, zr, ps, pr, zms, zmr, pms, pmr, fs, fr, xs, xr, xfs, xfr,
           os_, or_, ms_, mr_, bs, br, cs_, cr_, rs, rr):
    Z = E // 2
    HOP = Z // 4
    cap = 4 * rows // E
    blk = 2 * cap
    unit = width // sum(SHARES)
    hid = WG.shape[1]
    e = lax.axis_index("expert")
    x = lax.axis_index("tensor")
    c = lax.rem(e, 2)
    sgn = (1, -1)

    def at_z(k):
        return {"expert": lax.rem(e + 2 * k + 2 * E, E)}

    partner = {"expert": e + 1 - 2 * c}
    side_dev = ({"tensor": lax.rem(x + 1, NX)}, {"tensor": lax.rem(x + NX - 1, NX)})

    def cols(f):
        return slice(unit * sum(SHARES[:f]), unit * sum(SHARES[:f + 1]))

    def rcopy(src, dst, s, r, dev):
        return pltpu.make_async_remote_copy(src_ref=src, dst_ref=dst, send_sem=s, recv_sem=r,
                                            device_id=dev, device_id_type=MESH)

    def idx(d, j):
        return 0 if j == 0 else 2 * j - 1 + d

    def z_meta(d, j):
        return rcopy(M.at[idx(d, j), 0], M.at[idx(d, j + 1), 0],
                     zms.at[d, j], zmr.at[d, j], at_z(sgn[d]))

    def p_meta(o):
        return rcopy(M.at[o, 0], M.at[o, 1], pms.at[o], pmr.at[o], partner)

    def z_tok(d, j, f):
        return rcopy(T.at[idx(d, j), 0, :, cols(f)], T.at[idx(d, j + 1), 0, :, cols(f)], zs.at[d, j, f], zr.at[d, j, f], at_z(sgn[d]))

    def p_tok(o, f):
        return rcopy(T.at[o, 0, :, cols(f)], T.at[o, 1, :, cols(f)], ps.at[o, f], pr.at[o, f], partner)

    def far(d, i, f):
        if i == HOP:
            return rcopy(FS.at[c, i - 1, :, cols(f)], G.at[0, Z - 1, :, cols(f)],
                         fs.at[0, i - 1, f], fr.at[0, i - 1, f],
                         {"expert": lax.rem(e + 2 * i * (1 - 2 * c) + 2 * E, E)})
        return rcopy(FS.at[d, i - 1, :, cols(f)], G.at[0, idx(d, HOP + i), :, cols(f)],
                     fs.at[d, i - 1, f], fr.at[d, i - 1, f], at_z(sgn[d] * i))

    mid, NB = 2 * HOP + 1, Z
    groups = GROUPS
    near_g = [g for g in range(len(groups)) if groups[g][0] < mid]
    far_g = [g for g in range(len(groups)) if groups[g][0] >= mid]
    nears, fars = slice(0, mid), slice(mid, NB)

    def relayed(g):
        return [i for i in range(1, HOP + 1) if groups[g][0] <= 2 * (HOP + i) - 1 < groups[g][1]]

    def half(g, side):
        b0, b1 = groups[g]
        cut = (b0 + b1 + (b0 >= mid)) // 2
        return slice(b0, cut) if side == 0 else slice(cut, b1)

    def xsend(g, f, side):
        b, k, n = slice(*groups[g]), cols(f), g * PARTS + f
        return rcopy(G.at[0, b, :, k], G.at[1 + side, b, :, k], xs.at[n, side], xr.at[n, side], side_dev[side])

    def xfwd(g, f, side):
        b, k, n = half(g, side), cols(f), g * PARTS + f
        return rcopy(G.at[1 + side, b, :, k], G.at[3, b, :, k], xfs.at[n, side], xfr.at[n, side], side_dev[side])

    def opp(g, f, side):
        b, k, n = half(g, side), cols(f), g * PARTS + f
        return rcopy(PB.at[3, b, :, k], OPP.at[b, :, k], os_.at[n, side], or_.at[n, side], side_dev[side])

    def main(g, f, side):
        b, k, n = slice(*groups[g]), cols(f), g * PARTS + f
        return rcopy(PB.at[2 - side, b, :, k], RX.at[side, b, :, k], ms_.at[n, side], mr_.at[n, side], side_dev[side])

    def back(d, i, f):
        if i == HOP:
            return rcopy(R.at[Z - 1, :, cols(f)], FR.at[c, i - 1, :, cols(f)], bs.at[0, i - 1, f], br.at[0, i - 1, f],
                         {"expert": lax.rem(e - 2 * i * (1 - 2 * c) + 2 * E, E)})
        return rcopy(R.at[idx(d, HOP + i), :, cols(f)], FR.at[d, i - 1, :, cols(f)],
                     bs.at[d, i - 1, f], br.at[d, i - 1, f], at_z(-sgn[d] * i))

    def p_con(o, f):
        return rcopy(CP.at[o, :, cols(f)], CR.at[o, :, cols(f)], cs_.at[o, f], cr_.at[o, f], partner)

    def ring(d, j, f):
        return rcopy(C.at[idx(d, j), :, cols(f)], RZ.at[d, j - 1, :, cols(f)],
                     rs.at[d, j - 1, f], rr.at[d, j - 1, f], at_z(-sgn[d]))

    lane = lax.broadcasted_iota(jnp.int32, (1, 128), 1)

    def picks(o, n, first, scored):
        def both(r):
            return jnp.where(lane < rows, M[o, 0, r:r + 1, :], M[o, 1, r:r + 1, :])
        r = lax.broadcasted_iota(jnp.int32, (n * blk, 128), 0)
        ln = lax.broadcasted_iota(jnp.int32, (n * blk, 128), 1)
        ex = first(r // blk)
        ex = jnp.where(ex >= E, ex - E, ex)
        ex = jnp.where(ex < 0, ex + E, ex)
        slot = (cap * ex + lax.rem(r, cap)).astype(F32)
        mine = (lax.rem(r, blk) // cap) == (ln // rows)
        one = jnp.ones((n * blk, 128), F32)
        a, b = (both(2), both(3)) if scored else (one, one)
        val = jnp.where(both(0) == slot, a, 0.0) + jnp.where(both(1) == slot, b, 0.0)
        return jnp.where(mine, val, 0.0)[:, :2 * rows].astype(BF16)

    def own(o, scored):
        return picks(o, 1, lambda i: i + e, scored)

    def beyond(o, d, scored):
        return picks(o, HOP, lambda i: e + 2 * sgn[d] * (i + 1), scored)

    def select(lhs, o, f):
        return jnp.dot(lhs, T[o, :, :, cols(f)].reshape(2 * rows, -1), preferred_element_type=F32)

    kc = width // 6

    def ffn_in(b, f):
        n = NX * (b.stop - b.start) * blk
        lhs = G[:, b, :, cols(f)].reshape(n, -1)
        for m, W in ((0, WG), (1, WU)):
            got = jnp.dot(lhs, W[cols(f), :], preferred_element_type=F32)
            ACC[m, :, b] += got.reshape(NX, b.stop - b.start, blk, hid)

    def ffn_mid(b):
        gate = ACC[0, :, b]
        HID[:, b] = (gate / (1.0 + jnp.exp(-gate)) * ACC[1, :, b]).astype(BF16)

    def ffn_out(b, f):
        n = NX * (b.stop - b.start) * blk
        got = jnp.dot(HID[:, b].reshape(n, hid), WD[:, cols(f)], preferred_element_type=F32)
        PB[:, b, :, cols(f)] = got.astype(BF16).reshape(NX, b.stop - b.start, blk, -1)

    barrier = pltpu.get_barrier_semaphore()
    peers = [at_z(s * k) for k in range(1, HOP + 1) for s in sgn] + list(side_dev) + [partner]
    for dev in peers:
        pl.semaphore_signal(barrier, inc=1, device_id=dev, device_id_type=MESH)
    weights = [pltpu.make_async_copy(wg_in.at[0], WG, wsem.at[0]),
               pltpu.make_async_copy(wu_in.at[0], WU, wsem.at[1]),
               pltpu.make_async_copy(wd_in.at[0], WD, wsem.at[2])]
    for w in weights:
        w.start()

    row_t = lax.broadcasted_iota(jnp.int32, (rows, rows), 0)
    col_t = lax.broadcasted_iota(jnp.int32, (rows, rows), 1)
    named = [ids[k:k + 1, :].astype(F32) for k in (0, 1)]
    stood = [jnp.sum(jnp.where(row_t == col_t, r, 0.0), axis=1, keepdims=True) for r in named]
    M[0, 0] = jnp.zeros((8, 128), F32)
    for k in (0, 1):
        ahead = [jnp.where((q == named[k]) & (row_t < col_t), 1.0, 0.0) for q in stood]
        M[0, 0, k:k + 1, 0:rows] = named[k] * cap + jnp.sum(ahead[0] + ahead[1], axis=0, keepdims=True)
        M[0, 0, 2 + k:3 + k, 0:rows] = scores[k:k + 1, :]
    once = M[0, 0]
    M[0, 0] = jnp.where(lane < 2 * rows, once + pltpu.roll(once, rows, 1), -1.0)

    total = jnp.zeros((rows, 1), F32)
    for k in range(0, width, kc):
        t = tokens[:, k:k + kc].astype(F32)
        total = total + jnp.sum(t * t, axis=1, keepdims=True)
    scale = lax.rsqrt(total / width + 1e-05)
    for k in range(0, width, kc):
        T[0, 0, :, k:k + kc] = (tokens[:, k:k + kc].astype(F32) * scale * gain[:, k:k + kc]).astype(BF16)
    ACC[...] = jnp.zeros_like(ACC)
    FR[1 - c, HOP - 1] = jnp.zeros((blk, width), BF16)
    pl.semaphore_wait(barrier, len(peers))

    sent = []

    def go(make, *a):
        make(*a).start()
        sent.append((make, a))

    def weigh(lhs, rhs):
        return lax.dot_general(lhs, rhs, (((0,), (0,)), ((), ())), preferred_element_type=F32)

    seen = set()

    def new(*key):
        fresh = key not in seen
        seen.add(key)
        return fresh

    def launch(f):
        go(p_tok, 0, f)
        go(z_tok, 0, 0, f)
        go(z_tok, 1, 0, f)

    def hop(j, f):
        if new("hop", j):
            for d in (0, 1):
                z_meta(d, j - 1).wait_recv()
                if j < HOP:
                    go(z_meta, d, j)
                go(p_meta, idx(d, j))
        for d in (0, 1):
            z_tok(d, j - 1, f).wait_recv()
            if j < HOP:
                go(z_tok, d, j, f)
            go(p_tok, idx(d, j), f)

    def choose(j, f):
        for d in ((0, 1) if j > 0 else (0,)):
            o = idx(d, j)
            if new("choose", o):
                p_meta(o).wait_recv()
            lhs = own(o, False)
            if j == HOP:
                lhs = jnp.concatenate([lhs, beyond(o, d, False)], axis=0)
            p_tok(o, f).wait_recv()
            got = select(lhs, o, f).astype(BF16)
            G[0, o, :, cols(f)] = got[:blk]
            if j == HOP:
                FS[d, :, :, cols(f)] = got[blk:].reshape(HOP, blk, -1)
        if j == HOP:
            for i in range(1, HOP):
                for d in (0, 1):
                    go(far, d, i, f)
            go(far, 0, HOP, f)

    def spread(g, f):
        if g in far_g:
            for i in relayed(g):
                for d in ((0, 1) if i < HOP else (0,)):
                    far(d, i, f).wait_recv()
        for side in (0, 1):
            go(xsend, g, f, side)

    def forward(g, f):
        for side in (0, 1):
            xsend(g, f, side).wait_recv()
            go(xfwd, g, f, side)

    def layer_in(q, f):
        if new("weights"):
            for w in weights:
                w.wait()
        for g in (near_g, far_g)[q]:
            for side in (0, 1):
                xfwd(g, f, side).wait_recv()
        ffn_in((nears, fars)[q], f)

    def layer_mid(q):
        ffn_mid((nears, fars)[q])

    def layer_out(q, f):
        ffn_out((nears, fars)[q], f)

    def begin(g, f):
        for side in (0, 1):
            go(opp, g, f, side)

    def middle(g, f):
        k = cols(f)
        for side in (0, 1):
            b = half(g, side)
            opp(g, f, side).wait_recv()
            PB[2 - side, b, :, k] = (PB[2 - side, b, :, k].astype(F32) + OPP[b, :, k].astype(F32)).astype(BF16)
            go(main, g, f, side)

    def finish(g, f):
        b, k = slice(*groups[g]), cols(f)
        for side in (0, 1):
            main(g, f, side).wait_recv()
        R[b, :, k] = (PB[0, b, :, k].astype(F32) + RX[0, b, :, k].astype(F32) + RX[1, b, :, k].astype(F32)).astype(BF16)
        if g in far_g:
            for i in relayed(g)[::-1]:
                for d in ((0, 1) if i < HOP else (0,)):
                    go(back, d, i, f)

    def give(j, f):
        for d in ((0, 1) if j > 0 else (0,)):
            o = idx(d, j)
            u = weigh(own(o, True), R[o, :, cols(f)])
            if j == HOP:
                for i in range(1, HOP):
                    back(d, i, f).wait_recv()
                if d == 0:
                    back(0, HOP, f).wait_recv()
                u = u + weigh(beyond(o, d, True), FR[d, :, :, cols(f)].reshape(HOP * blk, -1))
            C[o, :, cols(f)] = u[:rows].astype(BF16)
            CP[o, :, cols(f)] = u[rows:].astype(BF16)
            go(p_con, o, f)

    def pass_on(j, f):
        for d in (0, 1):
            o = idx(d, j)
            p_con(o, f).wait_recv()
            v = C[o, :, cols(f)].astype(F32) + CR[o, :, cols(f)].astype(F32)
            if j < HOP:
                ring(d, j + 1, f).wait_recv()
                v = v + RZ[d, j, :, cols(f)].astype(F32)
            C[o, :, cols(f)] = v.astype(BF16)
            go(ring, d, j, f)

    def last(f):
        p_con(0, f).wait_recv()
        ring(0, 1, f).wait_recv()
        ring(1, 1, f).wait_recv()
        out[:, cols(f)] = (C[0, :, cols(f)].astype(F32) + CR[0, :, cols(f)].astype(F32)
                           + RZ[0, 0, :, cols(f)].astype(F32) + RZ[1, 0, :, cols(f)].astype(F32)).astype(BF16)

    for d in (0, 1):
        go(z_meta, d, 0)
    go(p_meta, 0)
    run = {"L": launch, "H": hop, "S": choose, "X": spread, "XF": forward, "FI": layer_in, "FM": layer_mid,
           "FO": layer_out, "O": begin, "M": middle, "N": finish, "G": give, "P": pass_on, "E": last}
    for task in ORDER:
        with jax.named_scope("_".join(map(str, task))):
            run[task[0]](*task[1:])
    for make, a in sent:
        make(*a).wait_send()


def on_device(tokens, expert_ids, gate_scores, norm_gain, w_gate, w_up, w_down):
    rows, width = tokens.shape
    E, NX = lax.axis_size("expert"), lax.axis_size("tensor")
    cap = 4 * rows // E
    Z, HOP, blk, hid = E // 2, E // 8, 2 * cap, w_gate.shape[2]
    NG, NO = len(GROUPS) * PARTS, 2 * HOP + 1
    v = lambda *s: pltpu.VMEM(s, BF16)
    return pl.pallas_call(
        functools.partial(kernel, E, NX, rows, width),
        out_shape=jax.ShapeDtypeStruct((rows, width), BF16),
        in_specs=[pl.BlockSpec(memory_space=pltpu.VMEM)] * 4 + [pl.BlockSpec(memory_space=pl.ANY)] * 3,
        out_specs=pl.BlockSpec(memory_space=pltpu.VMEM),
        scratch_shapes=[
            v(NO, 2, rows, width),
            pltpu.VMEM((NO, 2, 8, 128), F32),
            v(2, HOP, blk, width),
            v(NX, Z, blk, width),
            v(width, hid), v(width, hid), v(hid, width),
            pltpu.VMEM((2, NX, Z, blk, hid), F32),
            v(NX, Z, blk, hid),
            v(NX, Z, blk, width),
            v(Z, blk, width),
            v(2, Z, blk, width),
            v(Z, blk, width),
            v(2, HOP, blk, width),
            v(NO, rows, width), v(NO, rows, width), v(NO, rows, width),
            v(2, HOP, rows, width),
            DMA((3,)),
            DMA((2, HOP, PARTS)), DMA((2, HOP, PARTS)), DMA((NO, PARTS)), DMA((NO, PARTS)),
            DMA((2, HOP)), DMA((2, HOP)), DMA((NO,)), DMA((NO,)),
            DMA((2, HOP, PARTS)), DMA((2, HOP, PARTS)),
            DMA((NG, 2)), DMA((NG, 2)), DMA((NG, 2)), DMA((NG, 2)),
            DMA((NG, 2)), DMA((NG, 2)), DMA((NG, 2)), DMA((NG, 2)),
            DMA((2, HOP, PARTS)), DMA((2, HOP, PARTS)),
            DMA((NO, PARTS)), DMA((NO, PARTS)),
            DMA((2, HOP, PARTS)), DMA((2, HOP, PARTS)),
        ],
        compiler_params=pltpu.CompilerParams(collective_id=0, has_side_effects=True, vmem_limit_bytes=63 * 1024 * 1024),
    )(tokens, expert_ids.T, gate_scores.T, norm_gain.reshape(1, width), w_gate, w_up, w_down)


def solution(mesh):
    return jax.shard_map(
        on_device,
        mesh=mesh,
        in_specs=(
            P(("groups", "expert", "tensor"), None),
            P(("groups", "expert", "tensor"), None),
            P(("groups", "expert", "tensor"), None),
            P(),
            P("expert", None, "tensor"),
            P("expert", None, "tensor"),
            P("expert", "tensor", None),
        ),
        out_specs=P(("groups", "expert", "tensor"), None),
        check_vma=False,
    )
```

```python
import functools

import jax
import jax.numpy as jnp
from jax import lax
from jax.experimental import pallas as pl
from jax.experimental.pallas import tpu as pltpu
from jax.sharding import PartitionSpec as P

MESH = pl.DeviceIdType.MESH
F32, BF16 = jnp.float32, jnp.bfloat16
SHARES = (9, 9, 9, 9, 7, 5)
PARTS = len(SHARES)
GROUPS = ((0, 3), (3, 7), (7, 9), (9, 13), (13, 16))
DMA = pltpu.SemaphoreType.DMA
ORDER = [
    ("L", 0), ("L", 2), ("S", 0, 0), ("S", 0, 2), ("L", 1), ("S", 0, 1), ("H", 1, 0), ("S", 1, 0), ("X", 0, 0),
    ("H", 1, 2), ("S", 1, 2), ("X", 0, 2), ("H", 1, 1), ("S", 1, 1), ("X", 0, 1), ("H", 2, 0), ("XF", 0, 0),
    ("S", 2, 0), ("H", 2, 2), ("XF", 0, 2), ("S", 2, 2), ("H", 2, 1), ("XF", 0, 1), ("S", 2, 1), ("H", 3, 0),
    ("S", 3, 0), ("X", 1, 0), ("H", 3, 2), ("S", 3, 2), ("X", 1, 2), ("H", 3, 1), ("S", 3, 1), ("X", 1, 1),
    ("H", 4, 0), ("L", 3), ("XF", 1, 0), ("S", 4, 0), ("H", 4, 2), ("S", 0, 3), ("X", 2, 0), ("XF", 1, 2),
    ("S", 4, 2), ("H", 4, 1), ("X", 2, 2), ("XF", 1, 1), ("H", 1, 3), ("S", 4, 1), ("X", 2, 1), ("XF", 2, 0),
    ("S", 1, 3), ("X", 0, 3), ("X", 3, 0), ("XF", 2, 2), ("XF", 2, 1), ("FI", 0, 0), ("X", 3, 2), ("X", 4, 0),
    ("XF", 0, 3), ("XF", 3, 0), ("FI", 0, 2), ("H", 2, 3), ("FI", 0, 1), ("X", 4, 2), ("S", 2, 3), ("L", 5),
    ("XF", 3, 2), ("X", 3, 1), ("L", 4), ("S", 0, 5), ("XF", 4, 0), ("S", 0, 4), ("H", 3, 3), ("X", 4, 1),
    ("XF", 4, 2), ("H", 1, 5), ("S", 3, 3), ("X", 1, 3), ("S", 1, 5), ("H", 1, 4), ("X", 0, 5), ("XF", 3, 1),
    ("S", 1, 4), ("H", 4, 3), ("X", 0, 4), ("FI", 1, 0), ("H", 2, 5), ("S", 4, 3), ("XF", 4, 1), ("X", 2, 3),
    ("FI", 1, 2), ("H", 2, 4), ("S", 2, 5), ("S", 2, 4), ("XF", 1, 3), ("H", 3, 5), ("XF", 0, 5), ("S", 3, 5),
    ("X", 1, 5), ("X", 3, 3), ("XF", 0, 4), ("FI", 1, 1), ("XF", 2, 3), ("H", 3, 4), ("X", 4, 3), ("H", 4, 5),
    ("S", 3, 4), ("XF", 1, 5), ("X", 1, 4), ("S", 4, 5), ("X", 2, 5), ("XF", 3, 3), ("H", 4, 4), ("FI", 0, 3),
    ("S", 4, 4), ("X", 2, 4), ("XF", 4, 3), ("X", 3, 5), ("XF", 1, 4), ("XF", 2, 5), ("X", 4, 5), ("XF", 2, 4),
    ("X", 3, 4), ("FI", 1, 3), ("XF", 3, 5), ("FI", 0, 5), ("X", 4, 4), ("XF", 4, 5), ("FI", 0, 4), ("FM", 0),
    ("FO", 0, 0), ("O", 2, 0), ("FO", 0, 1), ("O", 1, 1), ("FO", 0, 2), ("XF", 3, 4), ("FO", 0, 3), ("FO", 0, 4),
    ("FO", 0, 5), ("O", 2, 4), ("XF", 4, 4), ("FI", 1, 5), ("O", 2, 1), ("M", 2, 0), ("M", 1, 1), ("M", 2, 4),
    ("FI", 1, 4), ("FM", 1), ("FO", 1, 0), ("FO", 1, 1), ("O", 4, 0), ("FO", 1, 2), ("M", 2, 1), ("FO", 1, 4),
    ("FO", 1, 5), ("N", 2, 0), ("FO", 1, 3), ("O", 4, 5), ("O", 3, 0), ("N", 1, 1), ("G", 2, 1), ("G", 3, 1),
    ("O", 4, 1), ("N", 2, 4), ("M", 4, 0), ("N", 2, 1), ("M", 4, 5), ("O", 3, 1), ("M", 3, 0), ("M", 4, 1),
    ("N", 4, 0), ("N", 4, 5), ("M", 3, 1), ("N", 3, 0), ("O", 3, 5), ("O", 4, 4), ("O", 3, 2), ("N", 4, 1),
    ("O", 3, 4), ("O", 4, 3), ("N", 3, 1), ("M", 3, 5), ("G", 4, 0), ("M", 4, 4), ("M", 3, 2), ("M", 3, 4),
    ("P", 4, 0), ("M", 4, 3), ("N", 3, 5), ("G", 4, 1), ("N", 4, 4), ("P", 4, 1), ("O", 4, 2), ("N", 3, 2),
    ("O", 3, 3), ("N", 3, 4), ("O", 2, 5), ("O", 1, 4), ("O", 2, 2), ("N", 4, 3), ("O", 2, 3), ("M", 4, 2),
    ("P", 3, 1), ("M", 3, 3), ("M", 2, 5), ("M", 1, 4), ("M", 2, 2), ("M", 2, 3), ("G", 4, 4), ("N", 4, 2),
    ("P", 4, 4), ("N", 3, 3), ("N", 2, 5), ("G", 4, 5), ("P", 2, 1), ("O", 1, 5), ("O", 1, 2), ("N", 1, 4),
    ("G", 3, 4), ("P", 4, 5), ("G", 2, 4), ("O", 1, 3), ("N", 2, 2), ("O", 1, 0), ("N", 2, 3), ("M", 1, 5),
    ("P", 3, 4), ("G", 4, 2), ("M", 1, 2), ("G", 4, 3), ("P", 4, 2), ("M", 1, 3), ("M", 1, 0), ("P", 4, 3),
    ("N", 1, 5), ("G", 3, 5), ("G", 2, 5), ("P", 3, 5), ("P", 2, 4), ("N", 1, 2), ("G", 2, 2), ("G", 3, 2),
    ("O", 0, 0), ("O", 0, 1), ("N", 1, 3), ("G", 3, 3), ("G", 2, 3), ("P", 3, 2), ("O", 0, 2), ("O", 0, 3),
    ("N", 1, 0), ("G", 2, 0), ("P", 3, 3), ("G", 3, 0), ("P", 2, 5), ("M", 0, 0), ("M", 0, 1), ("P", 3, 0),
    ("M", 0, 2), ("M", 0, 3), ("P", 2, 2), ("N", 0, 0), ("G", 0, 0), ("G", 1, 0), ("P", 2, 3), ("O", 0, 5),
    ("N", 0, 1), ("G", 1, 1), ("G", 0, 1), ("O", 0, 4), ("N", 0, 2), ("G", 1, 2), ("P", 1, 1), ("G", 0, 2),
    ("P", 2, 0), ("N", 0, 3), ("G", 1, 3), ("G", 0, 3), ("M", 0, 5), ("M", 0, 4), ("P", 1, 2), ("P", 1, 3),
    ("N", 0, 5), ("G", 0, 5), ("G", 1, 5), ("E", 1), ("N", 0, 4), ("G", 0, 4), ("G", 1, 4), ("P", 1, 5), ("P", 1, 0),
    ("P", 1, 4), ("E", 2), ("E", 3), ("E", 5), ("E", 0), ("E", 4),
]


def kernel(E, NX, rows, width, tokens, ids, scores, gain, wg_in, wu_in, wd_in, out,
           T, M, FS, G, WG, WU, WD, ACC, HID, PB, OPP, RX, R, FR, C, CP, CR, RZ,
           wsem, zs, zr, ps, pr, zms, zmr, pms, pmr, fs, fr, xs, xr, xfs, xfr,
           os_, or_, ms_, mr_, bs, br, cs_, cr_, rs, rr):
    Z = E // 2
    HOP = Z // 4
    cap = 4 * rows // E
    blk = 2 * cap
    unit = width // sum(SHARES)
    hid = WG.shape[1]
    e = lax.axis_index("expert")
    x = lax.axis_index("tensor")
    c = lax.rem(e, 2)
    sgn = (1, -1)

    def at_z(k):
        return {"expert": lax.rem(e + 2 * k + 2 * E, E)}

    partner = {"expert": e + 1 - 2 * c}
    side_dev = ({"tensor": lax.rem(x + 1, NX)}, {"tensor": lax.rem(x + NX - 1, NX)})

    def cols(f):
        return slice(unit * sum(SHARES[:f]), unit * sum(SHARES[:f + 1]))

    def rcopy(src, dst, s, r, dev):
        return pltpu.make_async_remote_copy(src_ref=src, dst_ref=dst, send_sem=s, recv_sem=r,
                                            device_id=dev, device_id_type=MESH)

    def idx(d, j):
        return 0 if j == 0 else 2 * j - 1 + d

    def z_meta(d, j):
        return rcopy(M.at[idx(d, j), 0], M.at[idx(d, j + 1), 0],
                     zms.at[d, j], zmr.at[d, j], at_z(sgn[d]))

    def p_meta(o):
        return rcopy(M.at[o, 0], M.at[o, 1], pms.at[o], pmr.at[o], partner)

    def z_tok(d, j, f):
        return rcopy(T.at[idx(d, j), 0, :, cols(f)], T.at[idx(d, j + 1), 0, :, cols(f)], zs.at[d, j, f], zr.at[d, j, f], at_z(sgn[d]))

    def p_tok(o, f):
        return rcopy(T.at[o, 0, :, cols(f)], T.at[o, 1, :, cols(f)], ps.at[o, f], pr.at[o, f], partner)

    def far(d, i, f):
        if i == HOP:
            return rcopy(FS.at[c, i - 1, :, cols(f)], G.at[0, Z - 1, :, cols(f)],
                         fs.at[0, i - 1, f], fr.at[0, i - 1, f],
                         {"expert": lax.rem(e + 2 * i * (1 - 2 * c) + 2 * E, E)})
        return rcopy(FS.at[d, i - 1, :, cols(f)], G.at[0, idx(d, HOP + i), :, cols(f)],
                     fs.at[d, i - 1, f], fr.at[d, i - 1, f], at_z(sgn[d] * i))

    mid, NB = 2 * HOP + 1, Z
    groups = GROUPS
    near_g = [g for g in range(len(groups)) if groups[g][0] < mid]
    far_g = [g for g in range(len(groups)) if groups[g][0] >= mid]
    nears, fars = slice(0, mid), slice(mid, NB)

    def relayed(g):
        return [i for i in range(1, HOP + 1) if groups[g][0] <= 2 * (HOP + i) - 1 < groups[g][1]]

    def half(g, side):
        b0, b1 = groups[g]
        cut = (b0 + b1 + (b0 >= mid)) // 2
        return slice(b0, cut) if side == 0 else slice(cut, b1)

    def xsend(g, f, side):
        b, k, n = slice(*groups[g]), cols(f), g * PARTS + f
        return rcopy(G.at[0, b, :, k], G.at[1 + side, b, :, k], xs.at[n, side], xr.at[n, side], side_dev[side])

    def xfwd(g, f, side):
        b, k, n = half(g, side), cols(f), g * PARTS + f
        return rcopy(G.at[1 + side, b, :, k], G.at[3, b, :, k], xfs.at[n, side], xfr.at[n, side], side_dev[side])

    def opp(g, f, side):
        b, k, n = half(g, side), cols(f), g * PARTS + f
        return rcopy(PB.at[3, b, :, k], OPP.at[b, :, k], os_.at[n, side], or_.at[n, side], side_dev[side])

    def main(g, f, side):
        b, k, n = slice(*groups[g]), cols(f), g * PARTS + f
        return rcopy(PB.at[2 - side, b, :, k], RX.at[side, b, :, k], ms_.at[n, side], mr_.at[n, side], side_dev[side])

    def back(d, i, f):
        if i == HOP:
            return rcopy(R.at[Z - 1, :, cols(f)], FR.at[c, i - 1, :, cols(f)], bs.at[0, i - 1, f], br.at[0, i - 1, f],
                         {"expert": lax.rem(e - 2 * i * (1 - 2 * c) + 2 * E, E)})
        return rcopy(R.at[idx(d, HOP + i), :, cols(f)], FR.at[d, i - 1, :, cols(f)],
                     bs.at[d, i - 1, f], br.at[d, i - 1, f], at_z(-sgn[d] * i))

    def p_con(o, f):
        return rcopy(CP.at[o, :, cols(f)], CR.at[o, :, cols(f)], cs_.at[o, f], cr_.at[o, f], partner)

    def ring(d, j, f):
        return rcopy(C.at[idx(d, j), :, cols(f)], RZ.at[d, j - 1, :, cols(f)],
                     rs.at[d, j - 1, f], rr.at[d, j - 1, f], at_z(-sgn[d]))

    lane = lax.broadcasted_iota(jnp.int32, (1, 128), 1)

    def picks(o, n, first, scored):
        def both(r):
            return jnp.where(lane < rows, M[o, 0, r:r + 1, :], M[o, 1, r:r + 1, :])
        r = lax.broadcasted_iota(jnp.int32, (n * blk, 128), 0)
        ln = lax.broadcasted_iota(jnp.int32, (n * blk, 128), 1)
        ex = first(r // blk)
        ex = jnp.where(ex >= E, ex - E, ex)
        ex = jnp.where(ex < 0, ex + E, ex)
        slot = (cap * ex + lax.rem(r, cap)).astype(F32)
        mine = (lax.rem(r, blk) // cap) == (ln // rows)
        one = jnp.ones((n * blk, 128), F32)
        a, b = (both(2), both(3)) if scored else (one, one)
        val = jnp.where(both(0) == slot, a, 0.0) + jnp.where(both(1) == slot, b, 0.0)
        return jnp.where(mine, val, 0.0)[:, :2 * rows].astype(BF16)

    def own(o, scored):
        return picks(o, 1, lambda i: i + e, scored)

    def beyond(o, d, scored):
        return picks(o, HOP, lambda i: e + 2 * sgn[d] * (i + 1), scored)

    def select(lhs, o, f):
        return jnp.dot(lhs, T[o, :, :, cols(f)].reshape(2 * rows, -1), preferred_element_type=F32)

    kc = width // 6

    def ffn_in(b, f):
        n = NX * (b.stop - b.start) * blk
        lhs = G[:, b, :, cols(f)].reshape(n, -1)
        for m, W in ((0, WG), (1, WU)):
            got = jnp.dot(lhs, W[cols(f), :], preferred_element_type=F32)
            ACC[m, :, b] += got.reshape(NX, b.stop - b.start, blk, hid)

    def ffn_mid(b):
        gate = ACC[0, :, b]
        HID[:, b] = (gate / (1.0 + jnp.exp(-gate)) * ACC[1, :, b]).astype(BF16)

    def ffn_out(b, f):
        n = NX * (b.stop - b.start) * blk
        got = jnp.dot(HID[:, b].reshape(n, hid), WD[:, cols(f)], preferred_element_type=F32)
        PB[:, b, :, cols(f)] = got.astype(BF16).reshape(NX, b.stop - b.start, blk, -1)

    barrier = pltpu.get_barrier_semaphore()
    peers = [at_z(s * k) for k in range(1, HOP + 1) for s in sgn] + list(side_dev) + [partner]
    for dev in peers:
        pl.semaphore_signal(barrier, inc=1, device_id=dev, device_id_type=MESH)
    weights = [pltpu.make_async_copy(wg_in.at[0], WG, wsem.at[0]),
               pltpu.make_async_copy(wu_in.at[0], WU, wsem.at[1]),
               pltpu.make_async_copy(wd_in.at[0], WD, wsem.at[2])]
    for w in weights:
        w.start()

    row_t = lax.broadcasted_iota(jnp.int32, (rows, rows), 0)
    col_t = lax.broadcasted_iota(jnp.int32, (rows, rows), 1)
    named = [ids[k:k + 1, :].astype(F32) for k in (0, 1)]
    stood = [jnp.sum(jnp.where(row_t == col_t, r, 0.0), axis=1, keepdims=True) for r in named]
    M[0, 0] = jnp.zeros((8, 128), F32)
    for k in (0, 1):
        ahead = [jnp.where((q == named[k]) & (row_t < col_t), 1.0, 0.0) for q in stood]
        M[0, 0, k:k + 1, 0:rows] = named[k] * cap + jnp.sum(ahead[0] + ahead[1], axis=0, keepdims=True)
        M[0, 0, 2 + k:3 + k, 0:rows] = scores[k:k + 1, :]
    once = M[0, 0]
    M[0, 0] = jnp.where(lane < 2 * rows, once + pltpu.roll(once, rows, 1), -1.0)

    total = jnp.zeros((rows, 1), F32)
    for k in range(0, width, kc):
        t = tokens[:, k:k + kc].astype(F32)
        total = total + jnp.sum(t * t, axis=1, keepdims=True)
    scale = lax.rsqrt(total / width + 1e-05)
    for k in range(0, width, kc):
        T[0, 0, :, k:k + kc] = (tokens[:, k:k + kc].astype(F32) * scale * gain[:, k:k + kc]).astype(BF16)
    ACC[...] = jnp.zeros_like(ACC)
    FR[1 - c, HOP - 1] = jnp.zeros((blk, width), BF16)
    pl.semaphore_wait(barrier, len(peers))

    sent = []

    def go(make, *a):
        make(*a).start()
        sent.append((make, a))

    def weigh(lhs, rhs):
        return lax.dot_general(lhs, rhs, (((0,), (0,)), ((), ())), preferred_element_type=F32)

    seen = set()

    def new(*key):
        fresh = key not in seen
        seen.add(key)
        return fresh

    def launch(f):
        go(p_tok, 0, f)
        go(z_tok, 0, 0, f)
        go(z_tok, 1, 0, f)

    def hop(j, f):
        if new("hop", j):
            for d in (0, 1):
                z_meta(d, j - 1).wait_recv()
                if j < HOP:
                    go(z_meta, d, j)
                go(p_meta, idx(d, j))
        for d in (0, 1):
            z_tok(d, j - 1, f).wait_recv()
            if j < HOP:
                go(z_tok, d, j, f)
            go(p_tok, idx(d, j), f)

    def choose(j, f):
        for d in ((0, 1) if j > 0 else (0,)):
            o = idx(d, j)
            if new("choose", o):
                p_meta(o).wait_recv()
            lhs = own(o, False)
            if j == HOP:
                lhs = jnp.concatenate([lhs, beyond(o, d, False)], axis=0)
            p_tok(o, f).wait_recv()
            got = select(lhs, o, f).astype(BF16)
            G[0, o, :, cols(f)] = got[:blk]
            if j == HOP:
                FS[d, :, :, cols(f)] = got[blk:].reshape(HOP, blk, -1)
        if j == HOP:
            for i in range(1, HOP):
                for d in (0, 1):
                    go(far, d, i, f)
            go(far, 0, HOP, f)

    def spread(g, f):
        if g in far_g:
            for i in relayed(g):
                for d in ((0, 1) if i < HOP else (0,)):
                    far(d, i, f).wait_recv()
        for side in (0, 1):
            go(xsend, g, f, side)

    def forward(g, f):
        for side in (0, 1):
            xsend(g, f, side).wait_recv()
            go(xfwd, g, f, side)

    def layer_in(q, f):
        if new("weights"):
            for w in weights:
                w.wait()
        for g in (near_g, far_g)[q]:
            for side in (0, 1):
                xfwd(g, f, side).wait_recv()
        ffn_in((nears, fars)[q], f)

    def layer_mid(q):
        ffn_mid((nears, fars)[q])

    def layer_out(q, f):
        ffn_out((nears, fars)[q], f)

    def begin(g, f):
        for side in (0, 1):
            go(opp, g, f, side)

    def middle(g, f):
        k = cols(f)
        for side in (0, 1):
            b = half(g, side)
            opp(g, f, side).wait_recv()
            PB[2 - side, b, :, k] = (PB[2 - side, b, :, k].astype(F32) + OPP[b, :, k].astype(F32)).astype(BF16)
            go(main, g, f, side)

    def finish(g, f):
        b, k = slice(*groups[g]), cols(f)
        for side in (0, 1):
            main(g, f, side).wait_recv()
        R[b, :, k] = (PB[0, b, :, k].astype(F32) + RX[0, b, :, k].astype(F32) + RX[1, b, :, k].astype(F32)).astype(BF16)
        if g in far_g:
            for i in relayed(g)[::-1]:
                for d in ((0, 1) if i < HOP else (0,)):
                    go(back, d, i, f)

    def give(j, f):
        for d in ((0, 1) if j > 0 else (0,)):
            o = idx(d, j)
            u = weigh(own(o, True), R[o, :, cols(f)])
            if j == HOP:
                for i in range(1, HOP):
                    back(d, i, f).wait_recv()
                if d == 0:
                    back(0, HOP, f).wait_recv()
                u = u + weigh(beyond(o, d, True), FR[d, :, :, cols(f)].reshape(HOP * blk, -1))
            C[o, :, cols(f)] = u[:rows].astype(BF16)
            CP[o, :, cols(f)] = u[rows:].astype(BF16)
            go(p_con, o, f)

    def pass_on(j, f):
        for d in (0, 1):
            o = idx(d, j)
            p_con(o, f).wait_recv()
            v = C[o, :, cols(f)].astype(F32) + CR[o, :, cols(f)].astype(F32)
            if j < HOP:
                ring(d, j + 1, f).wait_recv()
                v = v + RZ[d, j, :, cols(f)].astype(F32)
            C[o, :, cols(f)] = v.astype(BF16)
            go(ring, d, j, f)

    def last(f):
        p_con(0, f).wait_recv()
        ring(0, 1, f).wait_recv()
        ring(1, 1, f).wait_recv()
        out[:, cols(f)] = (C[0, :, cols(f)].astype(F32) + CR[0, :, cols(f)].astype(F32)
                           + RZ[0, 0, :, cols(f)].astype(F32) + RZ[1, 0, :, cols(f)].astype(F32)).astype(BF16)

    for d in (0, 1):
        go(z_meta, d, 0)
    go(p_meta, 0)
    run = {"L": launch, "H": hop, "S": choose, "X": spread, "XF": forward, "FI": layer_in, "FM": layer_mid,
           "FO": layer_out, "O": begin, "M": middle, "N": finish, "G": give, "P": pass_on, "E": last}
    first_out = [t[0] for t in ORDER].index("FO")
    early = 0
    for n, task in enumerate(ORDER):
        if n == first_out:
            early = len(sent)
        if task[0] == "E" and new("early"):
            for make, a in sent[:early]:
                make(*a).wait_send()
        with jax.named_scope("_".join(map(str, task))):
            run[task[0]](*task[1:])
    for make, a in sent[early:]:
        make(*a).wait_send()


def on_device(tokens, expert_ids, gate_scores, norm_gain, w_gate, w_up, w_down):
    rows, width = tokens.shape
    E, NX = lax.axis_size("expert"), lax.axis_size("tensor")
    cap = 4 * rows // E
    Z, HOP, blk, hid = E // 2, E // 8, 2 * cap, w_gate.shape[2]
    NG, NO = len(GROUPS) * PARTS, 2 * HOP + 1
    v = lambda *s: pltpu.VMEM(s, BF16)
    return pl.pallas_call(
        functools.partial(kernel, E, NX, rows, width),
        out_shape=jax.ShapeDtypeStruct((rows, width), BF16),
        in_specs=[pl.BlockSpec(memory_space=pltpu.VMEM)] * 4 + [pl.BlockSpec(memory_space=pl.ANY)] * 3,
        out_specs=pl.BlockSpec(memory_space=pltpu.VMEM),
        scratch_shapes=[
            v(NO, 2, rows, width),
            pltpu.VMEM((NO, 2, 8, 128), F32),
            v(2, HOP, blk, width),
            v(NX, Z, blk, width),
            v(width, hid), v(width, hid), v(hid, width),
            pltpu.VMEM((2, NX, Z, blk, hid), F32),
            v(NX, Z, blk, hid),
            v(NX, Z, blk, width),
            v(Z, blk, width),
            v(2, Z, blk, width),
            v(Z, blk, width),
            v(2, HOP, blk, width),
            v(NO, rows, width), v(NO, rows, width), v(NO, rows, width),
            v(2, HOP, rows, width),
            DMA((3,)),
            DMA((2, HOP, PARTS)), DMA((2, HOP, PARTS)), DMA((NO, PARTS)), DMA((NO, PARTS)),
            DMA((2, HOP)), DMA((2, HOP)), DMA((NO,)), DMA((NO,)),
            DMA((2, HOP, PARTS)), DMA((2, HOP, PARTS)),
            DMA((NG, 2)), DMA((NG, 2)), DMA((NG, 2)), DMA((NG, 2)),
            DMA((NG, 2)), DMA((NG, 2)), DMA((NG, 2)), DMA((NG, 2)),
            DMA((2, HOP, PARTS)), DMA((2, HOP, PARTS)),
            DMA((NO, PARTS)), DMA((NO, PARTS)),
            DMA((2, HOP, PARTS)), DMA((2, HOP, PARTS)),
        ],
        compiler_params=pltpu.CompilerParams(collective_id=0, has_side_effects=True, vmem_limit_bytes=63 * 1024 * 1024),
    )(tokens, expert_ids.T, gate_scores.T, norm_gain.reshape(1, width), w_gate, w_up, w_down)


def solution(mesh):
    return jax.shard_map(
        on_device,
        mesh=mesh,
        in_specs=(
            P(("groups", "expert", "tensor"), None),
            P(("groups", "expert", "tensor"), None),
            P(("groups", "expert", "tensor"), None),
            P(),
            P("expert", None, "tensor"),
            P("expert", None, "tensor"),
            P("expert", "tensor", None),
        ),
        out_specs=P(("groups", "expert", "tensor"), None),
        check_vma=False,
    )
```
